8 devices in a mesh: dp: 2 (over z, y), fo: 2 (over x), fi: 2 (over core).
Axes of the slice: x: 2, y: 2, z: 1, core: 2. Of those that a mesh axis runs over, the one named last changes fastest.
Arguments:
- X: bfloat16 [32768, 960], P(('dp', 'fo', 'fi'))
- dY: bfloat16 [32768, 960], P(('dp', 'fo', 'fi'))
- W1: bfloat16 [960, 2560], P(None, ('fo', 'fi'))
- W3: bfloat16 [960, 2560], P(None, ('fo', 'fi'))
- W2: bfloat16 [2560, 960], P(('fo', 'fi'))
- G: float32 [8, 3, 960, 2560], P(('dp', 'fo', 'fi'))
Outputs:
- output 1: bfloat16 [32768, 960], P(('dp', 'fo', 'fi'))
- output 2: float32 [3, 960, 2560], P(None, None, ('fo', 'fi'))
- output 3: float32 [8, 3, 960, 2560], P(('dp', 'fo', 'fi'))
All inputs are finite; a program needn't handle non-finite values.
Results may differ from the reference program's by a relative error of at most 0.00912588.
Values are sent between devices in bfloat16 or wider.
A program may use at most 1 GiB of HBM per device.

```python
import jax
import jax.numpy as jnp
from jax import lax

DEVS = 8
T = 4096
D = 960
FF = 2560


def setup_inputs(seed: int = 0) -> dict:
    key = jax.random.key(seed)
    k = jax.random.split(key, 6)
    n = DEVS * T
    x = jax.random.normal(k[0], (n, D), jnp.float32).astype(jnp.bfloat16)
    dy = jax.random.normal(k[1], (n, D), jnp.float32).astype(jnp.bfloat16)
    w1 = (jax.random.normal(k[2], (D, FF), jnp.float32) * D ** -0.5).astype(jnp.bfloat16)
    w3 = (jax.random.normal(k[3], (D, FF), jnp.float32) * D ** -0.5).astype(jnp.bfloat16)
    w2 = (jax.random.normal(k[4], (FF, D), jnp.float32) * FF ** -0.5).astype(jnp.bfloat16)
    g = jax.random.normal(k[5], (DEVS, 3, D, FF), jnp.float32)
    return {"X": x, "dY": dy, "W1": w1, "W3": w3, "W2": w2, "G": g}


def mlp_grads(x, dy, w1, w3, w2):
    a = jnp.dot(x, w1, preferred_element_type=jnp.float32)
    b = jnp.dot(x, w3, preferred_element_type=jnp.float32)
    s = jax.nn.sigmoid(a)
    sa = a * s
    h = (sa * b).astype(jnp.bfloat16)
    dh = jnp.dot(dy, w2.T, preferred_element_type=jnp.float32)
    da = (dh * b * (s * (1.0 + a * (1.0 - s)))).astype(jnp.bfloat16)
    db = (dh * sa).astype(jnp.bfloat16)
    dx = (jnp.dot(da, w1.T, preferred_element_type=jnp.float32)
          + jnp.dot(db, w3.T, preferred_element_type=jnp.float32)).astype(jnp.bfloat16)
    gw1 = jnp.dot(x.T, da, preferred_element_type=jnp.float32)
    gw3 = jnp.dot(x.T, db, preferred_element_type=jnp.float32)
    gw2 = jnp.dot(dy.T, h, preferred_element_type=jnp.float32)
    return dx, jnp.stack([gw1, gw3, gw2])


def reference(X, dY, W1, W3, W2, G):
    xs = X.reshape(DEVS, T, D)
    dys = dY.reshape(DEVS, T, D)
    dx, dwl = lax.map(lambda p: mlp_grads(p[0], p[1], W1, W3, W2), (xs, dys))
    dwn = jnp.sum(G.astype(jnp.bfloat16).astype(jnp.float32), axis=0)
    return dx.reshape(DEVS * T, D), dwn, dwl
```

```python
import functools

import jax
import jax.numpy as jnp
from jax import lax
from jax.experimental import pallas as pl
from jax.experimental.pallas import tpu as pltpu
from jax.sharding import PartitionSpec as P

BF = jnp.bfloat16
F32 = jnp.float32
T, D, FF = 4096, 960, 2560
SH = FF // 4
HB = FF // 2
TB = 512
NB = 256
VM = 62 * 1024 * 1024
ANY = pl.BlockSpec(memory_space=pl.ANY)


def load_shards(c, pairs, sem):
    cps = []
    for k, (mine, other, dst) in enumerate(pairs):
        cps.append(pltpu.make_async_copy(mine, dst.at[:, pl.ds(pl.multiple_of(c * SH, 128), SH)], sem.at[2 * k]))
        cps.append(pltpu.make_async_copy(other, dst.at[:, pl.ds(pl.multiple_of((1 - c) * SH, 128), SH)], sem.at[2 * k + 1]))
    for cp in cps:
        cp.start()
    for cp in cps:
        cp.wait()


def f_kernel(s_ref, x_ref, dy_ref, w1a, w1b, w3a, w3b, w2a, w2b, h_ref, da_ref, db_ref, w1, w3, w2, xt, dyt, sem):
    @pl.when(pl.program_id(0) == 0)
    def _():
        load_shards(s_ref[0], [(w1a, w1b, w1), (w3a, w3b, w3), (w2a, w2b, w2)], sem)

    xt[...] = x_ref[...].T
    dyt[...] = dy_ref[...].T
    for n in range(HB // NB):
        cs = slice(n * NB, (n + 1) * NB)
        a = jnp.dot(xt[...], w1[:, cs], preferred_element_type=F32)
        b = jnp.dot(xt[...], w3[:, cs], preferred_element_type=F32)
        dh = jnp.dot(dyt[...], w2[:, cs], preferred_element_type=F32)
        s = jax.nn.sigmoid(a)
        sa = a * s
        h_ref[:, cs] = (sa * b).astype(BF)
        da_ref[:, cs] = (dh * b * (s * (1.0 + a * (1.0 - s)))).astype(BF)
        db_ref[:, cs] = (dh * sa).astype(BF)


def f_call(c, xT, dyT, ws):
    out = jax.ShapeDtypeStruct((T, HB), BF)
    return pl.pallas_call(
        f_kernel,
        out_shape=(out, out, out),
        grid_spec=pltpu.PrefetchScalarGridSpec(
            num_scalar_prefetch=1, grid=(T // TB,),
            in_specs=[pl.BlockSpec((D, TB), lambda i, s: (0, i))] * 2 + [ANY] * 6,
            out_specs=[pl.BlockSpec((TB, HB), lambda i, s: (i, 0))] * 3,
            scratch_shapes=[pltpu.VMEM((D, HB), BF)] * 3 + [pltpu.VMEM((TB, D), BF)] * 2
            + [pltpu.SemaphoreType.DMA((6,))]),
        compiler_params=pltpu.CompilerParams(vmem_limit_bytes=VM),
        cost_estimate=pl.CostEstimate(flops=6 * T * D * HB, bytes_accessed=4 * T * D + 6 * T * HB + 6 * D * HB,
                                      transcendentals=T * HB),
    )(c, xT, dyT, *ws)


def gw_kernel(s_ref, x_ref, dy_ref, da_ref, db_ref, h_ref, *rest):
    o_ref = rest[-1]
    m = pl.program_id(0)

    @pl.when(m == 0)
    def _():
        o_ref[0, 0] = jnp.dot(x_ref[...], da_ref[...], preferred_element_type=F32)

    @pl.when(m == 1)
    def _():
        o_ref[0, 0] = jnp.dot(x_ref[...], db_ref[...], preferred_element_type=F32)

    @pl.when(m == 2)
    def _():
        o_ref[0, 0] = jnp.dot(dy_ref[...], h_ref[...], preferred_element_type=F32)


def gw_call(half, xT, dyT, da, db, h, acc):
    nj = HB // NB
    full = pl.BlockSpec((D, T), lambda m, j, s: (0, 0))

    def col(k):
        return pl.BlockSpec((T, NB), lambda m, j, s: (0, jnp.where(m == k, j, jnp.where(m < k, 0, nj - 1))))

    args = [half, xT, dyT, da, db, h]
    specs = [full, full, col(0), col(1), col(2)]
    alias = {}
    if acc is not None:
        args.append(acc)
        specs.append(ANY)
        alias = {6: 0}
    return pl.pallas_call(
        gw_kernel,
        out_shape=jax.ShapeDtypeStruct((1, 3, D, FF), F32),
        grid_spec=pltpu.PrefetchScalarGridSpec(
            num_scalar_prefetch=1, grid=(3, nj), in_specs=specs,
            out_specs=pl.BlockSpec((1, 1, D, NB), lambda m, j, s: (0, m, 0, s[0] * nj + j))),
        input_output_aliases=alias,
        compiler_params=pltpu.CompilerParams(vmem_limit_bytes=VM),
        cost_estimate=pl.CostEstimate(flops=6 * T * D * HB, bytes_accessed=4 * T * D + 6 * T * HB + 12 * D * HB,
                                      transcendentals=0),
    )(*args)


def dx_kernel(s_ref, da0, db0, da1, db1, *rest):
    wr, (o_ref, w1o, w3o, w1n, w3n, sem) = rest[:8], rest[8:]

    @pl.when(pl.program_id(0) == 0)
    def _():
        load_shards(s_ref[0], [(wr[0], wr[1], w1o), (wr[2], wr[3], w3o), (wr[4], wr[5], w1n), (wr[6], wr[7], w3n)], sem)

    def nt(w, d):
        return lax.dot_general(w[...], d[...], (((1,), (1,)), ((), ())), preferred_element_type=F32)

    o_ref[...] = (nt(w1o, da0) + nt(w3o, db0) + nt(w1n, da1) + nt(w3n, db1)).astype(BF)


def dx_call(c, acts, ws):
    return pl.pallas_call(
        dx_kernel,
        out_shape=jax.ShapeDtypeStruct((D, T), BF),
        grid_spec=pltpu.PrefetchScalarGridSpec(
            num_scalar_prefetch=1, grid=(T // TB,),
            in_specs=[pl.BlockSpec((TB, HB), lambda i, s: (i, 0))] * 4 + [ANY] * 8,
            out_specs=pl.BlockSpec((D, TB), lambda i, s: (0, i)),
            scratch_shapes=[pltpu.VMEM((D, HB), BF)] * 4 + [pltpu.SemaphoreType.DMA((8,))]),
        compiler_params=pltpu.CompilerParams(vmem_limit_bytes=VM),
        cost_estimate=pl.CostEstimate(flops=4 * T * D * FF, bytes_accessed=4 * T * FF + 4 * D * FF + 2 * T * D,
                                      transcendentals=0),
    )(c, *acts, *ws)


RB = 240


def cast_kernel(s_ref, g_ref, a_ref, b_ref, ea_ref, eb_ref):
    o, c = s_ref[0], s_ref[1]
    for ref, oo, cc in ((a_ref, o, c), (b_ref, 1 - o, c), (ea_ref, o, 1 - c), (eb_ref, 1 - o, 1 - c)):
        ref[...] = g_ref[0, 0, :, pl.ds(pl.multiple_of((oo * 2 + cc) * SH, 128), SH)].astype(BF)


def cast_call(oc, g, m):
    out = jax.ShapeDtypeStruct((D, SH), BF)
    return pl.pallas_call(
        cast_kernel,
        out_shape=(out,) * 4,
        grid_spec=pltpu.PrefetchScalarGridSpec(
            num_scalar_prefetch=1, grid=(D // RB,),
            in_specs=[pl.BlockSpec((1, 1, RB, FF), lambda i, s: (0, m, i, 0))],
            out_specs=[pl.BlockSpec((RB, SH), lambda i, s: (i, 0))] * 4),
        compiler_params=pltpu.CompilerParams(vmem_limit_bytes=VM),
        cost_estimate=pl.CostEstimate(flops=6 * D * FF, bytes_accessed=6 * D * FF, transcendentals=0),
    )(oc, g)


def solution(mesh):
    grp = ("fo", "fi")
    alla = ("dp", "fo", "fi")
    flip = [(0, 1), (1, 0)]

    def add(*v):
        return sum(t.astype(F32) for t in v)

    def local(x, dy, w1s, w3s, w2s, g):
        o, c = lax.axis_index("fo"), lax.axis_index("fi")
        oc = jnp.stack([o, c]).astype(jnp.int32)
        cv, ov, nv = oc[1:], oc[:1], 1 - oc[:1]
        xT, dyT = x.T, dy.T
        mine = [w1s, w3s, w2s.T]
        pair = [lax.ppermute(w, "fi", flip) for w in mine]
        far = [lax.ppermute(w, "fo", flip) for w in mine]
        farp = [lax.ppermute(w, "fi", flip) for w in far]
        own = [t for p in zip(mine, pair) for t in p]
        oth = [t for p in zip(far, farp) for t in p]

        parts = [cast_call(oc, g, m) for m in range(3)]
        a_in = [lax.ppermute(p[2], "fi", flip) for p in parts]
        b_in = [lax.ppermute(p[3], "fi", flip) for p in parts]
        h0, da0, db0 = f_call(cv, xT, dyT, own)
        bs = [add(parts[m][1], b_in[m]).astype(BF) for m in range(3)]
        x_in = [lax.ppermute(t, "fo", flip) for t in bs]
        acc = gw_call(ov, xT, dyT, da0, db0, h0, None)
        h1, da1, db1 = f_call(cv, xT, dyT, oth)
        gs = [add(parts[m][0], a_in[m], x_in[m]).astype(BF) for m in range(3)]
        y_in = [lax.ppermute(t, "dp", flip) for t in gs]
        dwl = gw_call(nv, xT, dyT, da1, db1, h1, acc)
        dxT = dx_call(cv, [da0, db0, da1, db1], own[:4] + oth[:4])
        dwn = jnp.stack([add(gs[m], y_in[m]) for m in range(3)])
        return dxT.T, dwn, dwl

    return jax.shard_map(
        local, mesh=mesh,
        in_specs=(P(alla, None), P(alla, None), P(None, grp), P(None, grp), P(grp, None),
                  P(alla, None, None, None)),
        out_specs=(P(alla, None), P(None, None, grp), P(alla, None, None, None)),
        check_vma=False)
```

```python
import functools

import jax
import jax.numpy as jnp
from jax import lax
from jax.experimental import pallas as pl
from jax.experimental.pallas import tpu as pltpu
from jax.sharding import PartitionSpec as P

BF = jnp.bfloat16
F32 = jnp.float32
T, D, FF = 4096, 960, 2560
SH = FF // 4
HB = FF // 2
TB = 512
NB = 256
VM = 62 * 1024 * 1024
ANY = pl.BlockSpec(memory_space=pl.ANY)


def load_shards(c, pairs, sem):
    cps = []
    for k, (mine, other, dst) in enumerate(pairs):
        cps.append(pltpu.make_async_copy(mine, dst.at[:, pl.ds(pl.multiple_of(c * SH, 128), SH)], sem.at[2 * k]))
        cps.append(pltpu.make_async_copy(other, dst.at[:, pl.ds(pl.multiple_of((1 - c) * SH, 128), SH)], sem.at[2 * k + 1]))
    for cp in cps:
        cp.start()
    for cp in cps:
        cp.wait()


def f_kernel(s_ref, x_ref, dy_ref, w1a, w1b, w3a, w3b, w2a, w2b, h_ref, da_ref, db_ref, w1, w3, w2, xt, dyt, sem):
    @pl.when(pl.program_id(0) == 0)
    def _():
        load_shards(s_ref[0], [(w1a, w1b, w1), (w3a, w3b, w3), (w2a, w2b, w2)], sem)

    xt[...] = x_ref[...].T
    dyt[...] = dy_ref[...].T
    for n in range(HB // NB):
        cs = slice(n * NB, (n + 1) * NB)
        a = jnp.dot(xt[...], w1[:, cs], preferred_element_type=F32)
        b = jnp.dot(xt[...], w3[:, cs], preferred_element_type=F32)
        dh = jnp.dot(dyt[...], w2[:, cs], preferred_element_type=F32)
        s = jax.nn.sigmoid(a)
        sa = a * s
        h_ref[:, cs] = (sa * b).astype(BF)
        da_ref[:, cs] = (dh * b * (s * (1.0 + a * (1.0 - s)))).astype(BF)
        db_ref[:, cs] = (dh * sa).astype(BF)


def f_call(c, xT, dyT, ws):
    out = jax.ShapeDtypeStruct((T, HB), BF)
    return pl.pallas_call(
        f_kernel,
        out_shape=(out, out, out),
        grid_spec=pltpu.PrefetchScalarGridSpec(
            num_scalar_prefetch=1, grid=(T // TB,),
            in_specs=[pl.BlockSpec((D, TB), lambda i, s: (0, i))] * 2 + [ANY] * 6,
            out_specs=[pl.BlockSpec((TB, HB), lambda i, s: (i, 0))] * 3,
            scratch_shapes=[pltpu.VMEM((D, HB), BF)] * 3 + [pltpu.VMEM((TB, D), BF)] * 2
            + [pltpu.SemaphoreType.DMA((6,))]),
        compiler_params=pltpu.CompilerParams(vmem_limit_bytes=VM),
        cost_estimate=pl.CostEstimate(flops=6 * T * D * HB, bytes_accessed=4 * T * D + 6 * T * HB + 6 * D * HB,
                                      transcendentals=T * HB),
    )(c, xT, dyT, *ws)


def gw_kernel(s_ref, x_ref, dy_ref, da_ref, db_ref, h_ref, *rest):
    o_ref = rest[-1]
    m = pl.program_id(0)

    @pl.when(m == 0)
    def _():
        o_ref[0, 0] = jnp.dot(x_ref[...], da_ref[...], preferred_element_type=F32)

    @pl.when(m == 1)
    def _():
        o_ref[0, 0] = jnp.dot(x_ref[...], db_ref[...], preferred_element_type=F32)

    @pl.when(m == 2)
    def _():
        o_ref[0, 0] = jnp.dot(dy_ref[...], h_ref[...], preferred_element_type=F32)


def gw_call(half, xT, dyT, da, db, h, acc):
    nj = HB // NB
    full = pl.BlockSpec((D, T), lambda m, j, s: (0, 0))

    def col(k):
        return pl.BlockSpec((T, NB), lambda m, j, s: (0, jnp.where(m == k, j, jnp.where(m < k, 0, nj - 1))))

    args = [half, xT, dyT, da, db, h]
    specs = [full, full, col(0), col(1), col(2)]
    alias = {}
    if acc is not None:
        args.append(acc)
        specs.append(ANY)
        alias = {6: 0}
    return pl.pallas_call(
        gw_kernel,
        out_shape=jax.ShapeDtypeStruct((1, 3, D, FF), F32),
        grid_spec=pltpu.PrefetchScalarGridSpec(
            num_scalar_prefetch=1, grid=(3, nj), in_specs=specs,
            out_specs=pl.BlockSpec((1, 1, D, NB), lambda m, j, s: (0, m, 0, s[0] * nj + j))),
        input_output_aliases=alias,
        compiler_params=pltpu.CompilerParams(vmem_limit_bytes=VM),
        cost_estimate=pl.CostEstimate(flops=6 * T * D * HB, bytes_accessed=4 * T * D + 6 * T * HB + 12 * D * HB,
                                      transcendentals=0),
    )(*args)


def dx_kernel(s_ref, da0, db0, da1, db1, *rest):
    wr, (o_ref, w1o, w3o, w1n, w3n, sem) = rest[:8], rest[8:]

    @pl.when(pl.program_id(0) == 0)
    def _():
        load_shards(s_ref[0], [(wr[0], wr[1], w1o), (wr[2], wr[3], w3o), (wr[4], wr[5], w1n), (wr[6], wr[7], w3n)], sem)

    def nt(w, d):
        return lax.dot_general(w[...], d[...], (((1,), (1,)), ((), ())), preferred_element_type=F32)

    o_ref[...] = (nt(w1o, da0) + nt(w3o, db0) + nt(w1n, da1) + nt(w3n, db1)).astype(BF)


def dx_call(c, acts, ws):
    return pl.pallas_call(
        dx_kernel,
        out_shape=jax.ShapeDtypeStruct((D, T), BF),
        grid_spec=pltpu.PrefetchScalarGridSpec(
            num_scalar_prefetch=1, grid=(T // TB,),
            in_specs=[pl.BlockSpec((TB, HB), lambda i, s: (i, 0))] * 4 + [ANY] * 8,
            out_specs=pl.BlockSpec((D, TB), lambda i, s: (0, i)),
            scratch_shapes=[pltpu.VMEM((D, HB), BF)] * 4 + [pltpu.SemaphoreType.DMA((8,))]),
        compiler_params=pltpu.CompilerParams(vmem_limit_bytes=VM),
        cost_estimate=pl.CostEstimate(flops=4 * T * D * FF, bytes_accessed=4 * T * FF + 4 * D * FF + 2 * T * D,
                                      transcendentals=0),
    )(c, *acts, *ws)


RB = 240


def cast_kernel(s_ref, g_ref, a_ref, b_ref, ea_ref, eb_ref):
    o, c = s_ref[0], s_ref[1]
    for ref, oo, cc in ((a_ref, o, c), (b_ref, 1 - o, c), (ea_ref, o, 1 - c), (eb_ref, 1 - o, 1 - c)):
        ref[...] = g_ref[0, 0, :, pl.ds(pl.multiple_of((oo * 2 + cc) * SH, 128), SH)].astype(BF)


def cast_call(oc, g, m):
    out = jax.ShapeDtypeStruct((D, SH), BF)
    return pl.pallas_call(
        cast_kernel,
        out_shape=(out,) * 4,
        grid_spec=pltpu.PrefetchScalarGridSpec(
            num_scalar_prefetch=1, grid=(D // RB,),
            in_specs=[pl.BlockSpec((1, 1, RB, FF), lambda i, s: (0, m, i, 0))],
            out_specs=[pl.BlockSpec((RB, SH), lambda i, s: (i, 0))] * 4),
        compiler_params=pltpu.CompilerParams(vmem_limit_bytes=VM),
        cost_estimate=pl.CostEstimate(flops=6 * D * FF, bytes_accessed=6 * D * FF, transcendentals=0),
    )(oc, g)


def final_kernel(g0, g1, g2, y0, y1, y2, o_ref):
    for m, (gr, yr) in enumerate(((g0, y0), (g1, y1), (g2, y2))):
        o_ref[m] = gr[...].astype(F32) + yr[...].astype(F32)


def final_call(gs, ys):
    return pl.pallas_call(
        final_kernel,
        out_shape=jax.ShapeDtypeStruct((3, D, SH), F32),
        grid=(D // RB,),
        in_specs=[pl.BlockSpec((RB, SH), lambda i: (i, 0))] * 6,
        out_specs=pl.BlockSpec((3, RB, SH), lambda i: (0, i, 0)),
        compiler_params=pltpu.CompilerParams(vmem_limit_bytes=16 * 1024 * 1024),
        cost_estimate=pl.CostEstimate(flops=3 * D * SH, bytes_accessed=24 * D * SH, transcendentals=0),
    )(*gs, *ys)


def solution(mesh):
    grp = ("fo", "fi")
    alla = ("dp", "fo", "fi")
    flip = [(0, 1), (1, 0)]

    def add(*v):
        return sum(t.astype(F32) for t in v)

    def local(x, dy, w1s, w3s, w2s, g):
        o, c = lax.axis_index("fo"), lax.axis_index("fi")
        oc = jnp.stack([o, c]).astype(jnp.int32)
        cv, ov, nv = oc[1:], oc[:1], 1 - oc[:1]
        xT, dyT = x.T, dy.T
        mine = [w1s, w3s, w2s.T]
        pair = [lax.ppermute(w, "fi", flip) for w in mine]
        far = [lax.ppermute(w, "fo", flip) for w in mine]
        own = [t for p in zip(mine, pair) for t in p]

        parts = [cast_call(oc, g, m) for m in range(3)]
        b_in = [lax.ppermute(p[3], "fi", flip) for p in parts]
        a_in = [lax.ppermute(p[2], "fi", flip) for p in parts]
        own, parts = lax.optimization_barrier((own, parts))
        h0, da0, db0 = f_call(cv, xT, dyT, own)
        b_in, far, h0 = lax.optimization_barrier((b_in, far, h0))
        farp = [lax.ppermute(w, "fi", flip) for w in far]
        oth = [t for p in zip(far, farp) for t in p]
        bs = [add(parts[m][1], b_in[m]).astype(BF) for m in range(3)]
        bs, h0 = lax.optimization_barrier((bs, h0))
        x_in = [lax.ppermute(t, "fo", flip) for t in bs]
        acc = gw_call(ov, xT, dyT, da0, db0, h0, None)
        oth, acc, x_in[0] = lax.optimization_barrier((oth, acc, x_in[0]))
        gs = [None] * 3
        gs[0] = add(parts[0][0], a_in[0], x_in[0]).astype(BF)
        oth, gs[0] = lax.optimization_barrier((oth, gs[0]))
        h1, da1, db1 = f_call(cv, xT, dyT, oth)
        h1, x_in[1], x_in[2] = lax.optimization_barrier((h1, x_in[1], x_in[2]))
        for m in (1, 2):
            gs[m] = add(parts[m][0], a_in[m], x_in[m]).astype(BF)
        gs[1], gs[2], h1, da1 = lax.optimization_barrier((gs[1], gs[2], h1, da1))
        y_in = [lax.ppermute(t, "dp", flip) for t in gs]
        dwl = gw_call(nv, xT, dyT, da1, db1, h1, acc)
        dxT = dx_call(cv, [da0, db0, da1, db1], own[:4] + oth[:4])
        y_in, dwl, dxT = lax.optimization_barrier((y_in, dwl, dxT))
        dwn = final_call(gs, y_in)
        return dxT.T, dwn, dwl

    return jax.shard_map(
        local, mesh=mesh,
        in_specs=(P(alla, None), P(alla, None), P(None, grp), P(None, grp), P(grp, None),
                  P(alla, None, None, None)),
        out_specs=(P(alla, None), P(None, None, grp), P(alla, None, None, None)),
        check_vma=False)
```

```python
import jax
import jax.numpy as jnp
from jax import lax
from jax.experimental import pallas as pl
from jax.experimental.pallas import tpu as pltpu
from jax.sharding import PartitionSpec as P

BF = jnp.bfloat16
F32 = jnp.float32
T, D, FF = 4096, 960, 2560
SH = FF // 4
HB = FF // 2
TB = 512
NT = T // TB
NB = 256
RC = 240
NK = 3 * D // RC
DH = D // 2
VM = 63 * 1024 * 1024
ANY = pl.BlockSpec(memory_space=pl.ANY)
DMA = pltpu.SemaphoreType.DMA


def rcopy(src, dst, ss, rs, dev):
    return pltpu.make_async_remote_copy(src_ref=src, dst_ref=dst, send_sem=ss, recv_sem=rs,
                                        device_id=dev, device_id_type=pl.DeviceIdType.MESH)


def main_kernel(x, dy, w1s, w3s, w2s, g,
                h, da, db, dxp, dx, rn, ra, gs,
                wo, wn, xb, yb, xt, yt, hb, dab, dbb, pb, ob, xs, xr, nb, ab, gb,
                wl, wcs, wcr, wxs, wxr, wys, wyr, w1fs, w1fr, w2fs, w2fr,
                gns, gnr, gas, gar, xss, xsr, ldn, lda, gst, xsem, hsem, psem, osem):
    d, o, c = lax.axis_index("dp"), lax.axis_index("fo"), lax.axis_index("fi")
    cdev, xdev, ydev = (d, o, 1 - c), (d, 1 - o, c), (1 - d, o, c)
    shards = (w1s, w3s, w2s)

    def cols(cc):
        return pl.ds(pl.multiple_of(cc * SH, 128), SH)

    def gcols(oo, cc):
        return pl.ds(pl.multiple_of((oo * 2 + cc) * SH, 128), SH)

    def rows(k):
        return pl.ds(pl.multiple_of(k * RC, 16), RC)

    def half(dd):
        return pl.ds(pl.multiple_of(dd * DH, 16), DH)

    bar = pltpu.get_barrier_semaphore()
    for dev in (cdev, xdev, ydev):
        pl.semaphore_signal(bar, inc=1, device_id=dev, device_id_type=pl.DeviceIdType.MESH)
    pl.semaphore_wait(bar, 3)

    def c_own(m):
        return rcopy(shards[m], wo.at[m, :, cols(c)], wcs.at[m], wcr.at[m], cdev)

    def x_own(m):
        return rcopy(shards[m].at[half(d), :], wn.at[m, half(d), cols(c)], wxs.at[m], wxr.at[m], xdev)

    def y_fwd(m):
        v = wn.at[m, half(d), cols(c)]
        return rcopy(v, v, wys.at[m], wyr.at[m], ydev)

    def c_fwd1(m):
        v = wn.at[m, half(d), cols(c)]
        return rcopy(v, v, w1fs.at[m], w1fr.at[m], cdev)

    def c_fwd2(m):
        v = wn.at[m, half(1 - d), cols(c)]
        return rcopy(v, v, w2fs.at[m], w2fr.at[m], cdev)

    def l_own(m):
        return pltpu.make_async_copy(shards[m], wo.at[m, :, cols(c)], wl.at[m])

    def g_n(k):
        return rcopy(g.at[rows(k), gcols(1 - o, 1 - c)], rn.at[rows(k), :], gns.at[k], gnr.at[k], cdev)

    def g_a(k):
        return rcopy(g.at[rows(k), gcols(o, 1 - c)], ra.at[rows(k), :], gas.at[k], gar.at[k], cdev)

    def x_sum(k):
        return rcopy(xs.at[k], xr.at[k], xss.at[k], xsr.at[k], xdev)

    def loads(k, oo, rec, buf, sem):
        q = k % 2
        return (pltpu.make_async_copy(g.at[rows(k), gcols(oo, c)], buf.at[q, 0], sem.at[q, 0]),
                pltpu.make_async_copy(rec.at[rows(k), :], buf.at[q, 1], sem.at[q, 1]))

    def load_n(k):
        return loads(k, 1 - o, rn, nb, ldn)

    def load_a(k):
        return loads(k, o, ra, ab, lda)

    def start_n(k):
        g_n(k).wait_recv()
        for cp in load_n(k):
            cp.start()

    def start_a(k):
        g_a(k).wait_recv()
        for cp in load_a(k):
            cp.start()

    def g_out(k):
        return pltpu.make_async_copy(gb.at[k % 2], gs.at[rows(k), :], gst.at[k % 2])

    def pair_sum(buf, q):
        return buf[q, 0].astype(BF).astype(F32) + buf[q, 1].astype(BF).astype(F32)

    def sum1(k):
        for cp in load_n(k):
            cp.wait()
        xs[k] = pair_sum(nb, k % 2).astype(BF)
        x_sum(k).start()

    def sum2(k):
        for cp in load_a(k):
            cp.wait()
        x_sum(k).wait_recv()
        gb[k % 2] = (pair_sum(ab, k % 2) + xr[k].astype(F32)).astype(BF)
        g_out(k).start()

    def tiles(j):
        q = j % 2
        t = pl.ds(pl.multiple_of((j % NT) * TB, 128), TB)
        return (pltpu.make_async_copy(x.at[:, t], xb.at[q], xsem.at[q, 0]),
                pltpu.make_async_copy(dy.at[:, t], yb.at[q], xsem.at[q, 1]))

    def acts(j):
        q = j % 2
        t = pl.ds(pl.multiple_of(j * TB, 128), TB)
        return (pltpu.make_async_copy(hb.at[q], h.at[t, :], hsem.at[q, 0]),
                pltpu.make_async_copy(dab.at[q], da.at[t, :], hsem.at[q, 1]),
                pltpu.make_async_copy(dbb.at[q], db.at[t, :], hsem.at[q, 2]))

    def tok(i):
        return pl.ds(pl.multiple_of(i * TB, 128), TB)

    def p_out(i):
        return pltpu.make_async_copy(pb.at[i % 2], dxp.at[:, tok(i)], psem.at[0, i % 2])

    def p_in(i):
        return pltpu.make_async_copy(dxp.at[:, tok(i)], pb.at[i % 2], psem.at[1, i % 2])

    def d_out(i):
        return pltpu.make_async_copy(ob.at[i % 2], dx.at[:, tok(i)], osem.at[i % 2])

    for m in range(3):
        l_own(m).start()
        c_own(m).start()
    for m in range(3):
        x_own(m).start()
    for cp in tiles(0):
        cp.start()

    @pl.loop(0, NK)
    def _(k):
        g_n(k).start()

    @pl.loop(0, NK)
    def _(k):
        g_a(k).start()

    for m in range(3):
        l_own(m).wait()
        c_own(m).wait_recv()

    def step(p, i):
        j = p * NT + i
        q = j % 2
        w = (wo, wn)[p]
        for cp in tiles(j):
            cp.wait()

        @pl.when(j < 2 * NT - 1)
        def _():
            for cp in tiles(j + 1):
                cp.start()

        if p == 0:
            for m, (s1, s2) in enumerate(((2, 4), (3, 6), (5, 8))):
                @pl.when(j == s1)
                def _():
                    y = x_own(m)
                    y.wait_recv()
                    y_fwd(m).start()
                    c_fwd1(m).start()

                if s2 < 8:
                    @pl.when(j == s2)
                    def _():
                        y_fwd(m).wait_recv()
                        c_fwd2(m).start()
        else:
            @pl.when(i < NT - 1)
            def _():
                p_in(i + 1).start()

        @pl.when((j >= 1) & (j < 1 + NK))
        def _():
            start_n(j - 1)

        @pl.when((j >= 2) & (j < 2 + NK))
        def _():
            sum1(j - 2)

        @pl.when(j >= 5)
        def _():
            start_a(j - 5)

        @pl.when(j >= 8)
        def _():
            g_out(j - 8).wait()

        @pl.when(j >= 6)
        def _():
            sum2(j - 6)

        def free():
            for cp in acts(j - 2):
                cp.wait()

        if p == 0:
            pl.when(i >= 2)(free)
        else:
            free()
        xt[...] = xb[q].T
        yt[...] = yb[q].T
        for n in range(HB // NB):
            cs = slice(n * NB, (n + 1) * NB)
            a = jnp.dot(xt[...], w[0, :, cs], preferred_element_type=F32)
            b = jnp.dot(xt[...], w[1, :, cs], preferred_element_type=F32)
            dh = jnp.dot(yt[...], w[2, :, cs], preferred_element_type=F32)
            s = jax.nn.sigmoid(a)
            sa = a * s
            hb[q, :, cs] = (sa * b).astype(BF)
            dab[q, :, cs] = (dh * b * (s * (1.0 + a * (1.0 - s)))).astype(BF)
            dbb[q, :, cs] = (dh * sa).astype(BF)
        for cp in acts(j):
            cp.start()

        def nt(m, v):
            return lax.dot_general(w[m], v[q], (((1,), (1,)), ((), ())), preferred_element_type=F32)

        if p == 0:
            @pl.when(i >= 2)
            def _():
                p_out(i - 2).wait()
            pb[q] = nt(0, dab) + nt(1, dbb)
            p_out(i).start()
        else:
            p_in(i).wait()

            @pl.when(i >= 2)
            def _():
                d_out(i - 2).wait()
            ob[q] = (pb[q] + nt(0, dab) + nt(1, dbb)).astype(BF)
            d_out(i).start()

    @pl.loop(0, NT)
    def _(i):
        step(0, i)

    for i in (NT - 2, NT - 1):
        p_out(i).wait()
    p_in(0).start()
    y_fwd(2).wait_recv()
    c_fwd2(2).start()
    for m in range(3):
        c_fwd1(m).wait_recv()
        c_fwd2(m).wait_recv()

    @pl.loop(0, NT)
    def _(i):
        step(1, i)

    start_a(NK - 1)
    for k in (NK - 2, NK - 1):
        g_out(k - 2).wait()
        sum2(k)
    for k in (NK - 2, NK - 1):
        g_out(k).wait()
    for i in (NT - 2, NT - 1):
        d_out(i).wait()
        for cp in acts(NT + i):
            cp.wait()
    for m in range(3):
        for f in (c_own, x_own, y_fwd, c_fwd1, c_fwd2):
            f(m).wait_send()

    @pl.loop(0, NK)
    def _(k):
        g_n(k).wait_send()
        g_a(k).wait_send()
        x_sum(k).wait_send()


def main_call(xT, dyT, w1s, w3s, w2sT, g2):
    act = jax.ShapeDtypeStruct((2 * T, HB), BF)
    outs = (act, act, act, jax.ShapeDtypeStruct((D, T), F32), jax.ShapeDtypeStruct((D, T), BF),
            jax.ShapeDtypeStruct((3 * D, SH), F32), jax.ShapeDtypeStruct((3 * D, SH), F32),
            jax.ShapeDtypeStruct((3 * D, SH), BF))
    V = pltpu.VMEM
    return pl.pallas_call(
        main_kernel,
        out_shape=outs,
        in_specs=[ANY] * 6,
        out_specs=(ANY,) * 8,
        scratch_shapes=[
            V((3, D, HB), BF), V((3, D, HB), BF),
            V((2, D, TB), BF), V((2, D, TB), BF), V((TB, D), BF), V((TB, D), BF),
            V((2, TB, HB), BF), V((2, TB, HB), BF), V((2, TB, HB), BF),
            V((2, D, TB), F32), V((2, D, TB), BF),
            V((NK, RC, SH), BF), V((NK, RC, SH), BF),
            V((2, 2, RC, SH), F32), V((2, 2, RC, SH), F32), V((2, RC, SH), BF),
        ] + [DMA((3,))] * 11 + [DMA((NK,))] * 6
        + [DMA((2, 2)), DMA((2, 2)), DMA((2,)), DMA((2, 2)), DMA((2, 3)), DMA((2, 2)), DMA((2,))],
        compiler_params=pltpu.CompilerParams(vmem_limit_bytes=VM, collective_id=0, has_side_effects=True),
        cost_estimate=pl.CostEstimate(flops=10 * T * D * FF, bytes_accessed=200_000_000, transcendentals=T * FF),
    )(xT, dyT, w1s, w3s, w2sT, g2)


def gw_kernel(s_ref, x_ref, dy_ref, da_ref, db_ref, h_ref, o_ref, xv, yv, sem):
    m, p, j = pl.program_id(0), pl.program_id(1), pl.program_id(2)
    cx = pltpu.make_async_copy(x_ref, xv, sem.at[0])
    cy = pltpu.make_async_copy(dy_ref, yv, sem.at[1])

    @pl.when((m == 0) & (p == 0) & (j == 0))
    def _():
        cx.start()
        cy.start()
        cx.wait()

    @pl.when((m == 2) & (p == 0) & (j == 0))
    def _():
        cy.wait()

    for k, (lhs, rhs) in enumerate(((xv, da_ref), (xv, db_ref), (yv, h_ref))):
        @pl.when(m == k)
        def _():
            o_ref[0, 0] = jnp.dot(lhs[...], rhs[...], preferred_element_type=F32)


def gw_call(ov, xT, dyT, da, db, h):
    nj = HB // NB

    def col(k):
        return pl.BlockSpec((T, NB), lambda m, p, j, s: (
            jnp.where(m == k, p, jnp.where(m < k, 0, 1)), jnp.where(m == k, j, jnp.where(m < k, 0, nj - 1))))

    return pl.pallas_call(
        gw_kernel,
        out_shape=jax.ShapeDtypeStruct((1, 3, D, FF), F32),
        grid_spec=pltpu.PrefetchScalarGridSpec(
            num_scalar_prefetch=1, grid=(3, 2, nj), in_specs=[ANY, ANY, col(0), col(1), col(2)],
            out_specs=pl.BlockSpec((1, 1, D, NB), lambda m, p, j, s: (0, m, 0, jnp.where(p == 0, s[0], 1 - s[0]) * nj + j)),
            scratch_shapes=[pltpu.VMEM((D, T), BF)] * 2 + [DMA((2,))]),
        compiler_params=pltpu.CompilerParams(vmem_limit_bytes=VM),
        cost_estimate=pl.CostEstimate(flops=6 * T * D * FF, bytes_accessed=4 * T * D + 6 * T * FF + 12 * D * FF,
                                      transcendentals=0),
    )(ov, xT, dyT, da, db, h)


def final_kernel(g_ref, y_ref, o_ref):
    o_ref[...] = g_ref[...].astype(F32) + y_ref[...].astype(F32)


def final_call(gs, ys):
    rb = 480
    spec = pl.BlockSpec((rb, SH), lambda i: (i, 0))
    return pl.pallas_call(
        final_kernel,
        out_shape=jax.ShapeDtypeStruct((3 * D, SH), F32),
        grid=(3 * D // rb,), in_specs=[spec, spec], out_specs=spec,
        compiler_params=pltpu.CompilerParams(vmem_limit_bytes=16 * 1024 * 1024),
        cost_estimate=pl.CostEstimate(flops=3 * D * SH, bytes_accessed=24 * D * SH, transcendentals=0),
    )(gs, ys)


def solution(mesh):
    grp = ("fo", "fi")
    alla = ("dp", "fo", "fi")
    flip = [(0, 1), (1, 0)]

    def local(x, dy, w1s, w3s, w2s, g):
        ov = lax.axis_index("fo").astype(jnp.int32).reshape(1)
        xT, dyT = x.T, dy.T
        h, da, db, _, dxT, _, _, gs = main_call(xT, dyT, w1s, w3s, w2s.T, g.reshape(3 * D, FF))
        ys = lax.ppermute(gs, "dp", flip)
        dwl = gw_call(ov, xT, dyT, da, db, h)
        ys, dwl = lax.optimization_barrier((ys, dwl))
        dwn = final_call(gs, ys).reshape(3, D, SH)
        return dxT.T, dwn, dwl

    return jax.shard_map(
        local, mesh=mesh,
        in_specs=(P(alla, None), P(alla, None), P(None, grp), P(None, grp), P(grp, None),
                  P(alla, None, None, None)),
        out_specs=(P(alla, None), P(None, None, grp), P(alla, None, None, None)),
        check_vma=False)
```

```python
import jax
import jax.numpy as jnp
from jax import lax
from jax.experimental import pallas as pl
from jax.experimental.pallas import tpu as pltpu
from jax.sharding import PartitionSpec as P

BF = jnp.bfloat16
F32 = jnp.float32
T, D, FF = 4096, 960, 2560
SH = FF // 4
HB = FF // 2
TB = 512
NT = T // TB
NB = 256
RC = 240
NK = 3 * D // RC
DH = D // 2
KY = 8
GB = 512
VM = 63 * 1024 * 1024
ANY = pl.BlockSpec(memory_space=pl.ANY)
DMA = pltpu.SemaphoreType.DMA


def rcopy(src, dst, ss, rs, dev):
    return pltpu.make_async_remote_copy(src_ref=src, dst_ref=dst, send_sem=ss, recv_sem=rs,
                                        device_id=dev, device_id_type=pl.DeviceIdType.MESH)


def main_kernel(x, dy, w1s, w3s, w2s, g,
                h, da, db, dxp, dx, rn, ra, gs, gt, ys,
                wo, wn, xb, yb, xt, yt, hb, dab, dbb, pb, ob, xs, xr, nb, ab, gb,
                wl, wcs, wcr, wxs, wxr, wys, wyr, w1fs, w1fr, w2fs, w2fr,
                gns, gnr, gas, gar, xss, xsr, yss, ysr, ldn, lda, gst, xsem, hsem, psem, osem):
    d, o, c = lax.axis_index("dp"), lax.axis_index("fo"), lax.axis_index("fi")
    cdev, xdev, ydev = (d, o, 1 - c), (d, 1 - o, c), (1 - d, o, c)
    shards = (w1s, w3s, w2s)

    def cols(cc):
        return pl.ds(pl.multiple_of(cc * SH, 128), SH)

    def gcols(oo, cc):
        return pl.ds(pl.multiple_of((oo * 2 + cc) * SH, 128), SH)

    def rows(k):
        return pl.ds(pl.multiple_of(k * RC, 16), RC)

    def half(dd):
        return pl.ds(pl.multiple_of(dd * DH, 16), DH)

    bar = pltpu.get_barrier_semaphore()
    for dev in (cdev, xdev, ydev):
        pl.semaphore_signal(bar, inc=1, device_id=dev, device_id_type=pl.DeviceIdType.MESH)
    pl.semaphore_wait(bar, 3)

    def c_own(m):
        return rcopy(shards[m], wo.at[m, :, cols(c)], wcs.at[m], wcr.at[m], cdev)

    def x_own(m):
        return rcopy(shards[m].at[half(d), :], wn.at[m, half(d), cols(c)], wxs.at[m], wxr.at[m], xdev)

    def y_fwd(m):
        v = wn.at[m, half(d), cols(c)]
        return rcopy(v, v, wys.at[m], wyr.at[m], ydev)

    def c_fwd1(m):
        v = wn.at[m, half(d), cols(c)]
        return rcopy(v, v, w1fs.at[m], w1fr.at[m], cdev)

    def c_fwd2(m):
        v = wn.at[m, half(1 - d), cols(c)]
        return rcopy(v, v, w2fs.at[m], w2fr.at[m], cdev)

    def l_own(m):
        return pltpu.make_async_copy(shards[m], wo.at[m, :, cols(c)], wl.at[m])

    def g_n(k):
        return rcopy(g.at[rows(k), gcols(1 - o, 1 - c)], rn.at[rows(k), :], gns.at[k], gnr.at[k], cdev)

    def g_a(k):
        return rcopy(g.at[rows(k), gcols(o, 1 - c)], ra.at[rows(k), :], gas.at[k], gar.at[k], cdev)

    def x_sum(k):
        return rcopy(xs.at[k], xr.at[k], xss.at[k], xsr.at[k], xdev)

    def loads(k, oo, rec, buf, sem):
        q = k % 2
        return (pltpu.make_async_copy(g.at[rows(k), gcols(oo, c)], buf.at[q, 0], sem.at[q, 0]),
                pltpu.make_async_copy(rec.at[rows(k), :], buf.at[q, 1], sem.at[q, 1]))

    def load_n(k):
        return loads(k, 1 - o, rn, nb, ldn)

    def load_a(k):
        return loads(k, o, ra, ab, lda)

    def start_n(k):
        g_n(k).wait_recv()
        for cp in load_n(k):
            cp.start()

    def start_a(k):
        g_a(k).wait_recv()
        for cp in load_a(k):
            cp.start()

    def g_out(k):
        return pltpu.make_async_copy(gb.at[k], gs.at[rows(k), :], gst.at[k])

    def t_out(k):
        return pltpu.make_async_copy(gb.at[k], gt.at[rows(k - KY), :], gst.at[k])

    def y_sum(k):
        return rcopy(gb.at[k], ys.at[rows(k), :], yss.at[k], ysr.at[k], ydev)

    def pair_sum(buf, q):
        return buf[q, 0].astype(BF).astype(F32) + buf[q, 1].astype(BF).astype(F32)

    def sum1(k, q):
        xs[k] = pair_sum(nb, q).astype(BF)

    def wait_a(k):
        for cp in load_a(k):
            cp.wait()
        x_sum(k).wait_recv()

    def sum2(k, q):
        gb[k] = (pair_sum(ab, q) + xr[k].astype(F32)).astype(BF)

    def share(k):
        g_out(k).start()
        y_sum(k).start()

    def tiles(j):
        q = j % 2
        t = pl.ds(pl.multiple_of((j % NT) * TB, 128), TB)
        return (pltpu.make_async_copy(x.at[:, t], xb.at[q], xsem.at[q, 0]),
                pltpu.make_async_copy(dy.at[:, t], yb.at[q], xsem.at[q, 1]))

    def acts(p, i):
        q = i % 2
        t = pl.ds(pl.multiple_of(i * TB, 128), TB)
        hc = pl.ds(pl.multiple_of((o if p == 0 else 1 - o) * HB, 128), HB)
        return (pltpu.make_async_copy(hb.at[q], h.at[t, hc], hsem.at[q, 0]),
                pltpu.make_async_copy(dab.at[q], da.at[t, hc], hsem.at[q, 1]),
                pltpu.make_async_copy(dbb.at[q], db.at[t, hc], hsem.at[q, 2]))

    def tok(i):
        return pl.ds(pl.multiple_of(i * TB, 128), TB)

    def p_out(i):
        return pltpu.make_async_copy(pb.at[i % 2], dxp.at[:, tok(i)], psem.at[0, i % 2])

    def p_in(i):
        return pltpu.make_async_copy(dxp.at[:, tok(i)], pb.at[i % 2], psem.at[1, i % 2])

    def d_out(i):
        return pltpu.make_async_copy(ob.at[i % 2], dx.at[:, tok(i)], osem.at[i % 2])

    def transpose(q):
        xt[...] = xb[q].T
        yt[...] = yb[q].T

    for m in range(3):
        c_own(m).start()
        l_own(m).start()
    for m in range(3):
        x_own(m).start()
    for t in (0, 1):
        for cp in tiles(t):
            cp.start()
    for cp in tiles(0):
        cp.wait()
    transpose(0)
    for m in range(3):
        l_own(m).wait()
        c_own(m).wait_recv()

    @pl.loop(0, NK)
    def _(k):
        g_n(k).start()

    @pl.loop(0, NK)
    def _(k):
        g_a(k).start()

    def step(p, i):
        j = p * NT + i
        q = i % 2
        w = (wo, wn)[p]

        def next_tile():
            for cp in tiles(j + 1):
                cp.wait()

        def start_tile():
            for cp in tiles(j + 2):
                cp.start()

        def free():
            for cp in acts(p, i):
                cp.wait()

        def wait_n():
            for cp in load_n(j - 2):
                cp.wait()

        if p == 0:
            next_tile()
            start_tile()
            for m, (s1, s2) in enumerate(((2, 5), (4, 7), (5, 8))):
                @pl.when(j == s1)
                def _():
                    x_own(m).wait_recv()
                    y_fwd(m).start()
                    c_fwd1(m).start()

                if s2 < 8:
                    @pl.when(j == s2)
                    def _():
                        y_fwd(m).wait_recv()
                        c_fwd2(m).start()

            @pl.when(i >= 2)
            def _():
                free()
                p_out(i - 2).wait()
                wait_n()

            @pl.when(i >= 1)
            def _():
                start_n(j - 1)

            @pl.when(i >= 5)
            def _():
                start_a(j - 5)

            @pl.when(i >= 6)
            def _():
                wait_a(j - 6)
                sum2(j - 6, q)
                share(j - 6)
        else:
            pl.when(i < NT - 1)(next_tile)
            pl.when(i < NT - 2)(start_tile)
            free()
            p_in(i).wait()

            @pl.when(i < NT - 1)
            def _():
                p_in(i + 1).start()

            @pl.when(i >= 2)
            def _():
                d_out(i - 2).wait()

            pl.when(i < NK + 2 - NT)(wait_n)

            @pl.when(i < NK + 1 - NT)
            def _():
                start_n(j - 1)

            start_a(j - 5)
            wait_a(j - 6)

        for n in range(HB // NB):
            cs = slice(n * NB, (n + 1) * NB)
            a = jnp.dot(xt[...], w[0, :, cs], preferred_element_type=F32)
            b = jnp.dot(xt[...], w[1, :, cs], preferred_element_type=F32)
            dh = jnp.dot(yt[...], w[2, :, cs], preferred_element_type=F32)
            s = jax.nn.sigmoid(a)
            sa = a * s
            hb[q, :, cs] = (sa * b).astype(BF)
            dab[q, :, cs] = (dh * b * (s * (1.0 + a * (1.0 - s)))).astype(BF)
            dbb[q, :, cs] = (dh * sa).astype(BF)

        def nt(m, v):
            return lax.dot_general(w[m], v[q], (((1,), (1,)), ((), ())), preferred_element_type=F32)

        transpose(1 - q)
        sum1((j + NK) % (NK + 2), q)
        if p == 0:
            pb[q] = nt(0, dab) + nt(1, dbb)
            p_out(i).start()
        else:
            sum2(j - 6, q)
            ob[q] = (pb[q] + nt(0, dab) + nt(1, dbb)).astype(BF)
            d_out(i).start()
        for cp in acts(p, i):
            cp.start()
        if p == 0:
            @pl.when(i >= 2)
            def _():
                x_sum(j - 2).start()
        else:
            @pl.when(i < NK + 2 - NT)
            def _():
                x_sum(j - 2).start()

            @pl.when(j - 6 < KY)
            def _():
                share(j - 6)

            @pl.when(j - 6 >= KY)
            def _():
                t_out(j - 6).start()

    @pl.loop(0, NT)
    def _(i):
        step(0, i)

    for i in (NT - 2, NT - 1):
        p_out(i).wait()
    p_in(0).start()
    y_fwd(2).wait_recv()
    c_fwd2(2).start()
    for m in range(3):
        c_fwd1(m).wait_recv()
        c_fwd2(m).wait_recv()

    @pl.loop(0, NT)
    def _(i):
        step(1, i)

    start_a(NK - 1)
    for k in (NK - 2, NK - 1):
        wait_a(k)
        sum2(k, k % 2)
        t_out(k).start()
    for i in (NT - 2, NT - 1):
        d_out(i).wait()
        for cp in acts(1, i):
            cp.wait()
    for m in range(3):
        for f in (c_own, x_own, y_fwd, c_fwd1, c_fwd2):
            f(m).wait_send()

    @pl.loop(0, NK)
    def _(k):
        g_n(k).wait_send()
        g_a(k).wait_send()
        x_sum(k).wait_send()

    @pl.loop(0, KY)
    def _(k):
        g_out(k).wait()
        y_sum(k).wait()

    for k in range(KY, NK):
        t_out(k).wait()


def main_call(xT, dyT, w1s, w3s, w2sT, g2):
    def out(n, m, t=BF):
        return jax.ShapeDtypeStruct((n, m), t)

    V = pltpu.VMEM
    return pl.pallas_call(
        main_kernel,
        out_shape=(out(T, FF), out(T, FF), out(T, FF), out(D, T, F32), out(D, T),
                   out(3 * D, SH, F32), out(3 * D, SH, F32),
                   out(KY * RC, SH), out((NK - KY) * RC, SH), out(KY * RC, SH)),
        in_specs=[ANY] * 6,
        out_specs=(ANY,) * 10,
        scratch_shapes=[
            V((3, D, HB), BF), V((3, D, HB), BF),
            V((2, D, TB), BF), V((2, D, TB), BF), V((TB, D), BF), V((TB, D), BF),
            V((2, TB, HB), BF), V((2, TB, HB), BF), V((2, TB, HB), BF),
            V((2, D, TB), F32), V((2, D, TB), BF),
            V((NK + 2, RC, SH), BF), V((NK, RC, SH), BF),
            V((2, 2, RC, SH), F32), V((2, 2, RC, SH), F32), V((NK, RC, SH), BF),
        ] + [DMA((3,))] * 11 + [DMA((NK,))] * 6 + [DMA((KY,))] * 2
        + [DMA((2, 2)), DMA((2, 2)), DMA((NK,)), DMA((2, 2)), DMA((2, 3)), DMA((2, 2)), DMA((2,))],
        compiler_params=pltpu.CompilerParams(vmem_limit_bytes=VM, collective_id=0, has_side_effects=True),
        cost_estimate=pl.CostEstimate(flops=10 * T * D * FF, bytes_accessed=200_000_000, transcendentals=T * FF),
    )(xT, dyT, w1s, w3s, w2sT, g2)


def gw_kernel(x_ref, dy_ref, da_ref, db_ref, h_ref, dxi_ref, g_ref, y_ref, o_ref, dxo_ref, s_ref, lhs, rb, lsem, rsem):
    nj = FF // GB
    s = pl.program_id(0)
    q = s % 2
    cx = pltpu.make_async_copy(x_ref, lhs.at[0], lsem.at[0])
    cy = pltpu.make_async_copy(dy_ref, lhs.at[1], lsem.at[1])

    def rhs(src, t):
        c = pl.ds(pl.multiple_of((t % nj) * GB, 128), GB)
        return pltpu.make_async_copy(src.at[:, c], rb.at[t % 2], rsem.at[t % 2])

    @pl.when(s == 0)
    def _():
        rhs(da_ref, s).start()
        cx.start()
        cx.wait()
        cy.start()

    for k, src in enumerate((da_ref, db_ref, h_ref)):
        @pl.when((s + 1 >= k * nj) & (s + 1 < (k + 1) * nj))
        def _():
            rhs(src, s + 1).start()

    @pl.when(s == 2 * nj)
    def _():
        cy.wait()

    rhs(da_ref, s).wait()
    o_ref[0, 0] = jnp.dot(lhs[s // (2 * nj)], rb[q], preferred_element_type=F32)
    dxo_ref[...] = dxi_ref[...]
    s_ref[...] = g_ref[...].astype(F32) + y_ref[...].astype(F32)


def gw_call(xT, dyT, da, db, h, dxi, gs, ys):
    nj = FF // GB
    dspec = pl.BlockSpec((D, TB), lambda s: (0, jnp.minimum(s, NT - 1)))
    gspec = pl.BlockSpec((RC, SH), lambda s: (jnp.minimum(s, KY - 1), 0))
    return pl.pallas_call(
        gw_kernel,
        out_shape=(jax.ShapeDtypeStruct((1, 3, D, FF), F32), jax.ShapeDtypeStruct((D, T), BF),
                   jax.ShapeDtypeStruct((3 * D, SH), F32)),
        grid=(3 * nj,),
        in_specs=[ANY] * 5 + [dspec, gspec, gspec],
        out_specs=(pl.BlockSpec((1, 1, D, GB), lambda s: (0, s // nj, 0, s % nj)), dspec, gspec),
        scratch_shapes=[pltpu.VMEM((2, D, T), BF), pltpu.VMEM((2, T, GB), BF), DMA((2,)), DMA((2,))],
        compiler_params=pltpu.CompilerParams(vmem_limit_bytes=VM),
        cost_estimate=pl.CostEstimate(flops=6 * T * D * FF, bytes_accessed=4 * T * D + 6 * T * FF + 12 * D * FF,
                                      transcendentals=0),
    )(xT, dyT, da, db, h, dxi, gs, ys)


def final_kernel(g_ref, y_ref, _, o_ref):
    o_ref[...] = g_ref[...].astype(F32) + y_ref[...].astype(F32)


def final_call(gt, yt, acc):
    rb, first = 480, KY * RC // 480
    spec = pl.BlockSpec((rb, SH), lambda i: (i, 0))
    return pl.pallas_call(
        final_kernel,
        out_shape=jax.ShapeDtypeStruct((3 * D, SH), F32),
        grid=((NK - KY) * RC // rb,), in_specs=[spec, spec, ANY],
        out_specs=pl.BlockSpec((rb, SH), lambda i: (i + first, 0)),
        input_output_aliases={2: 0},
        compiler_params=pltpu.CompilerParams(vmem_limit_bytes=16 * 1024 * 1024),
        cost_estimate=pl.CostEstimate(flops=D * SH, bytes_accessed=8 * D * SH, transcendentals=0),
    )(gt, yt, acc)


def solution(mesh):
    grp = ("fo", "fi")
    alla = ("dp", "fo", "fi")
    flip = [(0, 1), (1, 0)]

    def local(x, dy, w1s, w3s, w2s, g):
        xT, dyT = x.T, dy.T
        h, da, db, _, dxT, _, _, gs, gt, ys = main_call(xT, dyT, w1s, w3s, w2s.T, g.reshape(3 * D, FF))
        yt = lax.ppermute(gt, "dp", flip)
        dwl, dxT, dwn = gw_call(xT, dyT, da, db, h, dxT, gs, ys)
        yt, dwn = lax.optimization_barrier((yt, dwn))
        dwn = final_call(gt, yt, dwn).reshape(3, D, SH)
        return dxT.T, dwn, dwl

    return jax.shard_map(
        local, mesh=mesh,
        in_specs=(P(alla, None), P(alla, None), P(None, grp), P(None, grp), P(grp, None),
                  P(alla, None, None, None)),
        out_specs=(P(alla, None), P(None, None, grp), P(alla, None, None, None)),
        check_vma=False)
```

```python
import jax
import jax.numpy as jnp
from jax import lax
from jax.experimental import pallas as pl
from jax.experimental.pallas import tpu as pltpu
from jax.sharding import PartitionSpec as P

BF = jnp.bfloat16
F32 = jnp.float32
T, D, FF = 4096, 960, 2560
SH = FF // 4
HB = FF // 2
TB = 512
NT = T // TB
NB = 256
RC = 240
NK = 3 * D // RC
DH = D // 2
KY = 8
GB = 512
VM = 63 * 1024 * 1024
ANY = pl.BlockSpec(memory_space=pl.ANY)
DMA = pltpu.SemaphoreType.DMA


def rcopy(src, dst, ss, rs, dev):
    return pltpu.make_async_remote_copy(src_ref=src, dst_ref=dst, send_sem=ss, recv_sem=rs,
                                        device_id=dev, device_id_type=pl.DeviceIdType.MESH)


def main_kernel(x, dy, w1s, w3s, w2s, g,
                h, da, db, dxp, dx, rn, ra, gs, ys, ap, bp,
                wo, wn, xb, yb, xt, yt, hb, dab, dbb, pb, ob, xs, xr, nb, ab, gb,
                wl, wcs, wcr, wxs, wxr, wys, wyr, w1fs, w1fr, w2fs, w2fr,
                gns, gnr, gas, gar, xss, xsr, yss, ysr, ldn, lda, gst, bst, xsem, hsem, psem, osem):
    d, o, c = lax.axis_index("dp"), lax.axis_index("fo"), lax.axis_index("fi")
    cdev, xdev, ydev = (d, o, 1 - c), (d, 1 - o, c), (1 - d, o, c)
    shards = (w1s, w3s, w2s)

    def cols(cc):
        return pl.ds(pl.multiple_of(cc * SH, 128), SH)

    def gcols(oo, cc):
        return pl.ds(pl.multiple_of((oo * 2 + cc) * SH, 128), SH)

    def rows(k):
        return pl.ds(pl.multiple_of(k * RC, 16), RC)

    def half(dd):
        return pl.ds(pl.multiple_of(dd * DH, 16), DH)

    bar = pltpu.get_barrier_semaphore()
    for dev in (cdev, xdev, ydev):
        pl.semaphore_signal(bar, inc=1, device_id=dev, device_id_type=pl.DeviceIdType.MESH)
    pl.semaphore_wait(bar, 3)

    def c_own(m):
        return rcopy(shards[m], wo.at[m, :, cols(c)], wcs.at[m], wcr.at[m], cdev)

    def x_own(m):
        return rcopy(shards[m].at[half(d), :], wn.at[m, half(d), cols(c)], wxs.at[m], wxr.at[m], xdev)

    def y_fwd(m):
        v = wn.at[m, half(d), cols(c)]
        return rcopy(v, v, wys.at[m], wyr.at[m], ydev)

    def c_fwd1(m):
        v = wn.at[m, half(d), cols(c)]
        return rcopy(v, v, w1fs.at[m], w1fr.at[m], cdev)

    def c_fwd2(m):
        v = wn.at[m, half(1 - d), cols(c)]
        return rcopy(v, v, w2fs.at[m], w2fr.at[m], cdev)

    def l_own(m):
        return pltpu.make_async_copy(shards[m], wo.at[m, :, cols(c)], wl.at[m])

    def g_n(k):
        return rcopy(g.at[rows(k), gcols(1 - o, 1 - c)], rn.at[rows(k), :], gns.at[k], gnr.at[k], cdev)

    def g_a(k):
        return rcopy(g.at[rows(k), gcols(o, 1 - c)], ra.at[rows(k), :], gas.at[k], gar.at[k], cdev)

    def x_sum(k):
        return rcopy(xs.at[k], xr.at[k], xss.at[k], xsr.at[k], xdev)

    def loads(k, oo, rec, buf, sem):
        q = k % 2
        return (pltpu.make_async_copy(g.at[rows(k), gcols(oo, c)], buf.at[q, 0], sem.at[q, 0]),
                pltpu.make_async_copy(rec.at[rows(k), :], buf.at[q, 1], sem.at[q, 1]))

    def load_n(k):
        return loads(k, 1 - o, rn, nb, ldn)

    def load_a(k):
        return loads(k, o, ra, ab, lda)

    def start_n(k):
        g_n(k).wait_recv()
        for cp in load_n(k):
            cp.start()

    def start_a(k):
        g_a(k).wait_recv()
        for cp in load_a(k):
            cp.start()

    def g_out(k):
        return pltpu.make_async_copy(gb.at[k], gs.at[rows(k), :], gst.at[k])

    def a_out(k):
        return pltpu.make_async_copy(gb.at[k], ap.at[rows(k - KY), :], gst.at[k])

    def b_out(k):
        return pltpu.make_async_copy(xs.at[k], bp.at[rows(k - KY), :], bst.at[k - KY])

    def y_sum(k):
        return rcopy(gb.at[k], ys.at[rows(k), :], yss.at[k], ysr.at[k], ydev)

    def pair_sum(buf, q):
        return buf[q, 0].astype(BF).astype(F32) + buf[q, 1].astype(BF).astype(F32)

    def sum1(k, q):
        xs[k] = pair_sum(nb, q).astype(BF)

    def wait_a(k):
        for cp in load_a(k):
            cp.wait()

    def sum2(k, r, q):
        gb[k] = (pair_sum(ab, q) + xr[r].astype(F32)).astype(BF)

    def share(k):
        g_out(k).start()
        y_sum(k).start()

    def tiles(j):
        q = j % 2
        t = pl.ds(pl.multiple_of((j % NT) * TB, 128), TB)
        return (pltpu.make_async_copy(x.at[:, t], xb.at[q], xsem.at[q, 0]),
                pltpu.make_async_copy(dy.at[:, t], yb.at[q], xsem.at[q, 1]))

    def acts(p, i):
        q = i % 2
        t = pl.ds(pl.multiple_of(i * TB, 128), TB)
        hc = pl.ds(pl.multiple_of((o if p == 0 else 1 - o) * HB, 128), HB)
        return (pltpu.make_async_copy(hb.at[q], h.at[t, hc], hsem.at[q, 0]),
                pltpu.make_async_copy(dab.at[q], da.at[t, hc], hsem.at[q, 1]),
                pltpu.make_async_copy(dbb.at[q], db.at[t, hc], hsem.at[q, 2]))

    def tok(i):
        return pl.ds(pl.multiple_of(i * TB, 128), TB)

    def p_out(i):
        return pltpu.make_async_copy(pb.at[i % 2], dxp.at[:, tok(i)], psem.at[0, i % 2])

    def p_in(i):
        return pltpu.make_async_copy(dxp.at[:, tok(i)], pb.at[i % 2], psem.at[1, i % 2])

    def d_out(i):
        return pltpu.make_async_copy(ob.at[i % 2], dx.at[:, tok(i)], osem.at[i % 2])

    def transpose(q):
        xt[...] = xb[q].T
        yt[...] = yb[q].T

    for m in range(3):
        c_own(m).start()
        l_own(m).start()
    for m in range(3):
        x_own(m).start()
    for t in (0, 1):
        for cp in tiles(t):
            cp.start()
    for cp in tiles(0):
        cp.wait()
    transpose(0)
    for m in range(3):
        l_own(m).wait()
        c_own(m).wait_recv()

    for k in range(NK - KY):
        g_n(k).start()
        g_a(KY + k).start()
    for k in range(NK - KY, NK):
        g_n(k).start()
    for k in range(KY):
        g_a(k).start()

    def step(p, i):
        j = p * NT + i
        q = i % 2
        w = (wo, wn)[p]

        def next_tile():
            for cp in tiles(j + 1):
                cp.wait()

        def start_tile():
            for cp in tiles(j + 2):
                cp.start()

        def free():
            for cp in acts(p, i):
                cp.wait()

        def wait_n():
            for cp in load_n(j - 2):
                cp.wait()

        if p == 0:
            next_tile()
            start_tile()
            for m, (s1, s2) in enumerate(((2, 5), (4, 7), (5, 8))):
                @pl.when(j == s1)
                def _():
                    x_own(m).wait_recv()
                    y_fwd(m).start()
                    c_fwd1(m).start()

                if s2 < 8:
                    @pl.when(j == s2)
                    def _():
                        y_fwd(m).wait_recv()
                        c_fwd2(m).start()

            @pl.when(i >= 2)
            def _():
                free()
                p_out(i - 2).wait()
                wait_n()

            @pl.when(i >= 1)
            def _():
                start_n(j - 1)

            @pl.when((i >= 2) & (i < 2 + NK - KY))
            def _():
                wait_a(j + 6)

            @pl.when((i >= 1) & (i < 1 + NK - KY))
            def _():
                start_a(j + 7)

            @pl.when(i >= 5)
            def _():
                start_a(j - 5)

            @pl.when(i >= 6)
            def _():
                wait_a(j - 6)
                x_sum(j - 6).wait_recv()
                sum2(j - 6, j - 6, q)
                share(j - 6)
        else:
            pl.when(i < NT - 1)(next_tile)
            pl.when(i < NT - 2)(start_tile)
            free()
            p_in(i).wait()

            @pl.when(i < NT - 1)
            def _():
                p_in(i + 1).start()

            @pl.when(i >= 2)
            def _():
                d_out(i - 2).wait()

            pl.when(i < NK + 2 - NT)(wait_n)

            @pl.when(i < NK + 1 - NT)
            def _():
                start_n(j - 1)

            @pl.when(j < KY + 5)
            def _():
                start_a(j - 5)

            @pl.when(j < KY + 6)
            def _():
                wait_a(j - 6)
                x_sum(j - 6).wait_recv()

        for n in range(HB // NB):
            cs = slice(n * NB, (n + 1) * NB)
            a = jnp.dot(xt[...], w[0, :, cs], preferred_element_type=F32)
            b = jnp.dot(xt[...], w[1, :, cs], preferred_element_type=F32)
            dh = jnp.dot(yt[...], w[2, :, cs], preferred_element_type=F32)
            s = jax.nn.sigmoid(a)
            sa = a * s
            hb[q, :, cs] = (sa * b).astype(BF)
            dab[q, :, cs] = (dh * b * (s * (1.0 + a * (1.0 - s)))).astype(BF)
            dbb[q, :, cs] = (dh * sa).astype(BF)

        def nt(m, v):
            return lax.dot_general(w[m], v[q], (((1,), (1,)), ((), ())), preferred_element_type=F32)

        transpose(1 - q)
        sum1((j + NK) % (NK + 2), q)
        if p == 0:
            gb[j + 6] = pair_sum(ab, q).astype(BF)
            pb[q] = nt(0, dab) + nt(1, dbb)
            p_out(i).start()
        else:
            sum2(j - 6 + (NK - KY) * (j // (KY + 6)), (j - 6) % KY, q)
            ob[q] = (pb[q] + nt(0, dab) + nt(1, dbb)).astype(BF)
            d_out(i).start()
        for cp in acts(p, i):
            cp.start()
        if p == 0:
            @pl.when(i >= 2)
            def _():
                x_sum(j - 2).start()

            @pl.when((i >= 2) & (i < 2 + NK - KY))
            def _():
                a_out(j + 6).start()
        else:
            @pl.when(j < KY + 2)
            def _():
                x_sum(j - 2).start()

            @pl.when((j >= KY + 2) & (j < NK + 2))
            def _():
                b_out(j - 2).start()

            @pl.when(j < KY + 6)
            def _():
                share(j - 6)

    @pl.loop(0, NT)
    def _(i):
        step(0, i)

    for i in (NT - 2, NT - 1):
        p_out(i).wait()
    p_in(0).start()
    y_fwd(2).wait_recv()
    c_fwd2(2).start()
    for m in range(3):
        c_fwd1(m).wait_recv()
        c_fwd2(m).wait_recv()

    @pl.loop(0, NT)
    def _(i):
        step(1, i)

    for i in (NT - 2, NT - 1):
        d_out(i).wait()
        for cp in acts(1, i):
            cp.wait()
    for m in range(3):
        for f in (c_own, x_own, y_fwd, c_fwd1, c_fwd2):
            f(m).wait_send()

    @pl.loop(0, NK)
    def _(k):
        g_n(k).wait_send()
        g_a(k).wait_send()

    @pl.loop(0, KY)
    def _(k):
        x_sum(k).wait_send()
        g_out(k).wait()
        y_sum(k).wait()

    for k in range(KY, NK):
        a_out(k).wait()
        b_out(k).wait()


def main_call(xT, dyT, w1s, w3s, w2sT, g2):
    def out(n, m, t=BF):
        return jax.ShapeDtypeStruct((n, m), t)

    V = pltpu.VMEM
    return pl.pallas_call(
        main_kernel,
        out_shape=(out(T, FF), out(T, FF), out(T, FF), out(D, T, F32), out(D, T),
                   out(3 * D, SH, F32), out(3 * D, SH, F32),
                   out(KY * RC, SH), out(KY * RC, SH), out((NK - KY) * RC, SH), out((NK - KY) * RC, SH)),
        in_specs=[ANY] * 6,
        out_specs=(ANY,) * 11,
        scratch_shapes=[
            V((3, D, HB), BF), V((3, D, HB), BF),
            V((2, D, TB), BF), V((2, D, TB), BF), V((TB, D), BF), V((TB, D), BF),
            V((2, TB, HB), BF), V((2, TB, HB), BF), V((2, TB, HB), BF),
            V((2, D, TB), F32), V((2, D, TB), BF),
            V((NK + 2, RC, SH), BF), V((KY, RC, SH), BF),
            V((2, 2, RC, SH), F32), V((2, 2, RC, SH), F32), V((NK + 2, RC, SH), BF),
        ] + [DMA((3,))] * 11 + [DMA((NK,))] * 4 + [DMA((KY,))] * 4
        + [DMA((2, 2)), DMA((2, 2)), DMA((NK,)), DMA((NK - KY,)), DMA((2, 2)), DMA((2, 3)), DMA((2, 2)), DMA((2,))],
        compiler_params=pltpu.CompilerParams(vmem_limit_bytes=VM, collective_id=0, has_side_effects=True),
        cost_estimate=pl.CostEstimate(flops=10 * T * D * FF, bytes_accessed=200_000_000, transcendentals=T * FF),
    )(xT, dyT, w1s, w3s, w2sT, g2)


def gw_kernel(x_ref, dy_ref, da_ref, db_ref, h_ref, dxi_ref, g_ref, y_ref, o_ref, dxo_ref, s_ref, lhs, rb, lsem, rsem):
    nj = FF // GB
    s = pl.program_id(0)
    q = s % 2
    cx = pltpu.make_async_copy(x_ref, lhs.at[0], lsem.at[0])
    cy = pltpu.make_async_copy(dy_ref, lhs.at[1], lsem.at[1])

    def rhs(src, t):
        c = pl.ds(pl.multiple_of((t % nj) * GB, 128), GB)
        return pltpu.make_async_copy(src.at[:, c], rb.at[t % 2], rsem.at[t % 2])

    @pl.when(s == 0)
    def _():
        rhs(da_ref, s).start()
        cx.start()
        cx.wait()
        cy.start()

    for k, src in enumerate((da_ref, db_ref, h_ref)):
        @pl.when((s + 1 >= k * nj) & (s + 1 < (k + 1) * nj))
        def _():
            rhs(src, s + 1).start()

    @pl.when(s == 2 * nj)
    def _():
        cy.wait()

    rhs(da_ref, s).wait()
    o_ref[0, 0] = jnp.dot(lhs[s // (2 * nj)], rb[q], preferred_element_type=F32)
    dxo_ref[...] = dxi_ref[...]
    s_ref[...] = g_ref[...].astype(F32) + y_ref[...].astype(F32)


def gw_call(xT, dyT, da, db, h, dxi, gs, ys):
    nj = FF // GB
    dspec = pl.BlockSpec((D, TB), lambda s: (0, jnp.minimum(s, NT - 1)))
    gspec = pl.BlockSpec((RC, SH), lambda s: (jnp.minimum(s, KY - 1), 0))
    return pl.pallas_call(
        gw_kernel,
        out_shape=(jax.ShapeDtypeStruct((1, 3, D, FF), F32), jax.ShapeDtypeStruct((D, T), BF),
                   jax.ShapeDtypeStruct((3 * D, SH), F32)),
        grid=(3 * nj,),
        in_specs=[ANY] * 5 + [dspec, gspec, gspec],
        out_specs=(pl.BlockSpec((1, 1, D, GB), lambda s: (0, s // nj, 0, s % nj)), dspec, gspec),
        scratch_shapes=[pltpu.VMEM((2, D, T), BF), pltpu.VMEM((2, T, GB), BF), DMA((2,)), DMA((2,))],
        compiler_params=pltpu.CompilerParams(vmem_limit_bytes=VM),
        cost_estimate=pl.CostEstimate(flops=6 * T * D * FF, bytes_accessed=4 * T * D + 6 * T * FF + 12 * D * FF,
                                      transcendentals=0),
    )(xT, dyT, da, db, h, dxi, gs, ys)


def final_kernel(a_ref, x_ref, y_ref, z_ref, _, o_ref):
    o_ref[...] = (a_ref[...].astype(F32) + x_ref[...].astype(F32)) + (y_ref[...].astype(F32) + z_ref[...].astype(F32))


def final_call(terms, acc):
    rb, first = 480, KY * RC // 480
    spec = pl.BlockSpec((rb, SH), lambda i: (i, 0))
    return pl.pallas_call(
        final_kernel,
        out_shape=jax.ShapeDtypeStruct((3 * D, SH), F32),
        grid=((NK - KY) * RC // rb,), in_specs=[spec] * 4 + [ANY],
        out_specs=pl.BlockSpec((rb, SH), lambda i: (i + first, 0)),
        input_output_aliases={4: 0},
        compiler_params=pltpu.CompilerParams(vmem_limit_bytes=VM),
        cost_estimate=pl.CostEstimate(flops=D * SH, bytes_accessed=8 * D * SH, transcendentals=0),
    )(*terms, acc)


def solution(mesh):
    grp = ("fo", "fi")
    alla = ("dp", "fo", "fi")
    flip = [(0, 1), (1, 0)]

    def local(x, dy, w1s, w3s, w2s, g):
        xT, dyT = x.T, dy.T
        h, da, db, _, dxT, _, _, gs, ys, ap, bp = main_call(xT, dyT, w1s, w3s, w2s.T, g.reshape(3 * D, FF))
        far = [lax.ppermute(bp, "fo", flip), lax.ppermute(ap, "dp", flip),
               lax.ppermute(bp, ("dp", "fo"), [(k, 3 - k) for k in range(4)])]
        dwl, dxT, dwn = gw_call(xT, dyT, da, db, h, dxT, gs, ys)
        far, dwn = lax.optimization_barrier((far, dwn))
        dwn = final_call([ap] + far, dwn).reshape(3, D, SH)
        return dxT.T, dwn, dwl

    return jax.shard_map(
        local, mesh=mesh,
        in_specs=(P(alla, None), P(alla, None), P(None, grp), P(None, grp), P(grp, None),
                  P(alla, None, None, None)),
        out_specs=(P(alla, None), P(None, None, grp), P(alla, None, None, None)),
        check_vma=False)
```

```python
import jax
import jax.numpy as jnp
from jax import lax
from jax.experimental import pallas as pl
from jax.experimental.pallas import tpu as pltpu
from jax.sharding import PartitionSpec as P

BF = jnp.bfloat16
F32 = jnp.float32
T, D, FF = 4096, 960, 2560
SH = FF // 4
HB = FF // 2
TB = 512
NT = T // TB
NB = 256
RC = 240
NK = 3 * D // RC
DH = D // 2
KY = 8
GB = 512
VM = 63 * 1024 * 1024
ANY = pl.BlockSpec(memory_space=pl.ANY)
DMA = pltpu.SemaphoreType.DMA


def rcopy(src, dst, ss, rs, dev):
    return pltpu.make_async_remote_copy(src_ref=src, dst_ref=dst, send_sem=ss, recv_sem=rs,
                                        device_id=dev, device_id_type=pl.DeviceIdType.MESH)


def main_kernel(x, dy, w1s, w3s, w2s, g,
                act, dxp, dx, rn, ra, gs, gt, ys,
                wo, wn, xb, yb, xt, yt, hb, dab, dbb, pb, ob, xs, xr, nb, ab, gb,
                wl, wcs, wcr, wxs, wxr, wys, wyr, w1fs, w1fr, w2fs, w2fr,
                gns, gnr, gas, gar, xss, xsr, yss, ysr, ldn, lda, gst, xsem, hsem, psem, osem):
    d, o, c = lax.axis_index("dp"), lax.axis_index("fo"), lax.axis_index("fi")
    cdev, xdev, ydev = (d, o, 1 - c), (d, 1 - o, c), (1 - d, o, c)
    shards = (w1s, w3s, w2s)

    mine, other = slice(0, SH), slice(SH, HB)

    def gcols(oo, cc):
        return pl.ds(pl.multiple_of((oo * 2 + cc) * SH, 128), SH)

    def rows(k):
        return pl.ds(pl.multiple_of(k * RC, 16), RC)

    def half(dd):
        return pl.ds(pl.multiple_of(dd * DH, 16), DH)

    bar = pltpu.get_barrier_semaphore()
    for dev in (cdev, xdev, ydev):
        pl.semaphore_signal(bar, inc=1, device_id=dev, device_id_type=pl.DeviceIdType.MESH)
    pl.semaphore_wait(bar, 3)

    def c_own(m):
        return rcopy(shards[m], wo.at[m, :, other], wcs.at[m], wcr.at[m], cdev)

    def x_own(m):
        return rcopy(shards[m].at[half(d), :], wn.at[m, half(d), mine], wxs.at[m], wxr.at[m], xdev)

    def y_fwd(m):
        v = wn.at[m, half(d), mine]
        return rcopy(v, v, wys.at[m], wyr.at[m], ydev)

    def c_fwd1(m):
        return rcopy(wn.at[m, half(d), mine], wn.at[m, half(d), other], w1fs.at[m], w1fr.at[m], cdev)

    def c_fwd2(m):
        return rcopy(wn.at[m, half(1 - d), mine], wn.at[m, half(1 - d), other], w2fs.at[m], w2fr.at[m], cdev)

    def l_own(m):
        return pltpu.make_async_copy(shards[m], wo.at[m, :, mine], wl.at[m])

    def g_n(k):
        return rcopy(g.at[rows(k), gcols(1 - o, 1 - c)], rn.at[rows(k), :], gns.at[k], gnr.at[k], cdev)

    def g_a(k):
        return rcopy(g.at[rows(k), gcols(o, 1 - c)], ra.at[rows(k), :], gas.at[k], gar.at[k], cdev)

    def x_sum(k):
        return rcopy(xs.at[k], xr.at[k], xss.at[k], xsr.at[k], xdev)

    def loads(k, oo, rec, buf, sem):
        q = k % 2
        return (pltpu.make_async_copy(g.at[rows(k), gcols(oo, c)], buf.at[q, 0], sem.at[q, 0]),
                pltpu.make_async_copy(rec.at[rows(k), :], buf.at[q, 1], sem.at[q, 1]))

    def load_n(k):
        return loads(k, 1 - o, rn, nb, ldn)

    def load_a(k):
        return loads(k, o, ra, ab, lda)

    def start_n(k):
        g_n(k).wait_recv()
        for cp in load_n(k):
            cp.start()

    def start_a(k):
        g_a(k).wait_recv()
        for cp in load_a(k):
            cp.start()

    def g_out(k):
        return pltpu.make_async_copy(gb.at[k], gs.at[rows(k), :], gst.at[k])

    def t_out(k):
        return pltpu.make_async_copy(gb.at[k], gt.at[rows(k - KY), :], gst.at[k])

    def y_sum(k):
        return rcopy(gb.at[k], ys.at[rows(k), :], yss.at[k], ysr.at[k], ydev)

    def pair_sum(buf, q):
        return buf[q, 0].astype(BF) + buf[q, 1].astype(BF)

    def sum1(k, q):
        xs[k] = pair_sum(nb, q)

    def wait_a(k):
        for cp in load_a(k):
            cp.wait()
        x_sum(k).wait_recv()

    def sum2(k, q):
        gb[k] = pair_sum(ab, q) + xr[k]

    def share(k):
        g_out(k).start()
        y_sum(k).start()

    def tiles(j):
        q = j % 2
        t = pl.ds(pl.multiple_of((j % NT) * TB, 128), TB)
        return (pltpu.make_async_copy(x.at[:, t], xb.at[q], xsem.at[q, 0]),
                pltpu.make_async_copy(dy.at[:, t], yb.at[q], xsem.at[q, 1]))

    def acts(p, i):
        q = i % 2
        t = pl.ds(pl.multiple_of(i * TB, 128), TB)
        oo = o if p == 0 else 1 - o
        return [pltpu.make_async_copy(v.at[q, :, loc], act.at[m, t, gcols(oo, cc)], hsem.at[q, m, k])
                for m, v in enumerate((dab, dbb, hb)) for k, (loc, cc) in enumerate(((mine, c), (other, 1 - c)))]

    def tok(i):
        return pl.ds(pl.multiple_of(i * TB, 128), TB)

    def p_out(i):
        return pltpu.make_async_copy(pb.at[i % 2], dxp.at[:, tok(i)], psem.at[0, i % 2])

    def p_in(i):
        return pltpu.make_async_copy(dxp.at[:, tok(i)], pb.at[i % 2], psem.at[1, i % 2])

    def d_out(i):
        return pltpu.make_async_copy(ob.at[i % 2], dx.at[:, tok(i)], osem.at[i % 2])

    def transpose(q):
        xt[...] = xb[q].T
        yt[...] = yb[q].T

    for m in range(3):
        c_own(m).start()
        l_own(m).start()
    for m in range(3):
        x_own(m).start()
    for t in (0, 1):
        for cp in tiles(t):
            cp.start()
    for cp in tiles(0):
        cp.wait()
    transpose(0)
    for m in range(3):
        l_own(m).wait()

    def shard_in():
        for m in range(3):
            c_own(m).wait_recv()

        @pl.loop(0, NK)
        def _(k):
            g_n(k).start()

        @pl.loop(0, NK)
        def _(k):
            g_a(k).start()

    def step(p, i):
        j = p * NT + i
        q = i % 2
        w = (wo, wn)[p]

        def next_tile():
            for cp in tiles(j + 1):
                cp.wait()

        def start_tile():
            for cp in tiles(j + 2):
                cp.start()

        def free():
            for cp in acts(p, i):
                cp.wait()

        def wait_n():
            for cp in load_n(j - 2):
                cp.wait()

        if p == 0:
            next_tile()
            start_tile()
            for m, (s1, s2) in enumerate(((2, 5), (4, 7), (5, 8))):
                @pl.when(j == s1)
                def _():
                    x_own(m).wait_recv()
                    y_fwd(m).start()
                    c_fwd1(m).start()

                if s2 < 8:
                    @pl.when(j == s2)
                    def _():
                        y_fwd(m).wait_recv()
                        c_fwd2(m).start()

            @pl.when(i >= 2)
            def _():
                free()
                p_out(i - 2).wait()
                wait_n()

            @pl.when(i >= 1)
            def _():
                start_n(j - 1)

            @pl.when(i >= 5)
            def _():
                start_a(j - 5)

            @pl.when(i >= 6)
            def _():
                wait_a(j - 6)
                sum2(j - 6, q)
                share(j - 6)
        else:
            pl.when(i < NT - 1)(next_tile)
            pl.when(i < NT - 2)(start_tile)
            free()
            p_in(i).wait()

            @pl.when(i < NT - 1)
            def _():
                p_in(i + 1).start()

            @pl.when(i >= 2)
            def _():
                d_out(i - 2).wait()

            pl.when(i < NK + 2 - NT)(wait_n)

            @pl.when(i < NK + 1 - NT)
            def _():
                start_n(j - 1)

            start_a(j - 5)
            wait_a(j - 6)

        for n in range(HB // NB):
            if p == 0 and n == 2:
                pl.when(j == 0)(shard_in)
            cs = slice(n * NB, (n + 1) * NB)
            a = jnp.dot(xt[...], w[0, :, cs], preferred_element_type=F32)
            b = jnp.dot(xt[...], w[1, :, cs], preferred_element_type=F32)
            dh = jnp.dot(yt[...], w[2, :, cs], preferred_element_type=F32)
            s = jax.nn.sigmoid(a)
            sa = a * s
            hb[q, :, cs] = (sa * b).astype(BF)
            dab[q, :, cs] = (dh * b * (s * (1.0 + a * (1.0 - s)))).astype(BF)
            dbb[q, :, cs] = (dh * sa).astype(BF)

        def nt(m, v):
            return lax.dot_general(w[m], v[q], (((1,), (1,)), ((), ())), preferred_element_type=F32)

        transpose(1 - q)
        sum1((j + NK) % (NK + 2), q)
        if p == 0:
            pb[q] = nt(0, dab) + nt(1, dbb)
            p_out(i).start()
        else:
            sum2(j - 6, q)
            ob[q] = (pb[q] + nt(0, dab) + nt(1, dbb)).astype(BF)
            d_out(i).start()
        for cp in acts(p, i):
            cp.start()
        if p == 0:
            @pl.when(i >= 2)
            def _():
                x_sum(j - 2).start()
        else:
            @pl.when(i < NK + 2 - NT)
            def _():
                x_sum(j - 2).start()

            @pl.when(j - 6 < KY)
            def _():
                share(j - 6)

            @pl.when(j - 6 >= KY)
            def _():
                t_out(j - 6).start()

    @pl.loop(0, NT)
    def _(i):
        step(0, i)

    for i in (NT - 2, NT - 1):
        p_out(i).wait()
    p_in(0).start()
    y_fwd(2).wait_recv()
    c_fwd2(2).start()
    for m in range(3):
        c_fwd1(m).wait_recv()
        c_fwd2(m).wait_recv()

    @pl.loop(0, NT)
    def _(i):
        step(1, i)

    start_a(NK - 1)
    for k in (NK - 2, NK - 1):
        wait_a(k)
        sum2(k, k % 2)
        t_out(k).start()
    for i in (NT - 2, NT - 1):
        d_out(i).wait()
        for cp in acts(1, i):
            cp.wait()
    for m in range(3):
        for f in (c_own, x_own, y_fwd, c_fwd1, c_fwd2):
            f(m).wait_send()

    @pl.loop(0, NK)
    def _(k):
        g_n(k).wait_send()
        g_a(k).wait_send()
        x_sum(k).wait_send()

    @pl.loop(0, KY)
    def _(k):
        g_out(k).wait()
        y_sum(k).wait()

    for k in range(KY, NK):
        t_out(k).wait()


def main_call(xT, dyT, w1s, w3s, w2sT, g2):
    def out(n, m, t=BF):
        return jax.ShapeDtypeStruct((n, m), t)

    V = pltpu.VMEM
    return pl.pallas_call(
        main_kernel,
        out_shape=(jax.ShapeDtypeStruct((3, T, FF), BF), out(D, T, F32), out(D, T),
                   out(3 * D, SH, F32), out(3 * D, SH, F32),
                   out(KY * RC, SH), out((NK - KY) * RC, SH), out(KY * RC, SH)),
        in_specs=[ANY] * 6,
        out_specs=(ANY,) * 8,
        scratch_shapes=[
            V((3, D, HB), BF), V((3, D, HB), BF),
            V((2, D, TB), BF), V((2, D, TB), BF), V((TB, D), BF), V((TB, D), BF),
            V((2, TB, HB), BF), V((2, TB, HB), BF), V((2, TB, HB), BF),
            V((2, D, TB), F32), V((2, D, TB), BF),
            V((NK + 2, RC, SH), BF), V((NK, RC, SH), BF),
            V((2, 2, RC, SH), F32), V((2, 2, RC, SH), F32), V((NK, RC, SH), BF),
        ] + [DMA((3,))] * 11 + [DMA((NK,))] * 6 + [DMA((KY,))] * 2
        + [DMA((2, 2)), DMA((2, 2)), DMA((NK,)), DMA((2, 2)), DMA((2, 3, 2)), DMA((2, 2)), DMA((2,))],
        compiler_params=pltpu.CompilerParams(vmem_limit_bytes=VM, collective_id=0, has_side_effects=True),
        cost_estimate=pl.CostEstimate(flops=10 * T * D * FF, bytes_accessed=200_000_000, transcendentals=T * FF),
    )(xT, dyT, w1s, w3s, w2sT, g2)


def gw_kernel(x, dy, act, dxi, gs, ys, dwl, dxo, dwn, lhs, rb, ob, dv, gv, sv, xsem, fsem, ysem, rsem, osem, dsem, gsem, ssem):
    nj, nk, ni, ns = FF // GB, 4, 7, 6
    kc = T // nk

    def col(s):
        return pl.ds(pl.multiple_of(s % nj * GB, 128), GB)

    def x_in(k):
        return pltpu.make_async_copy(x.at[:, k * kc:(k + 1) * kc], lhs.at[0, :, k * kc:(k + 1) * kc], xsem.at[k])

    def first_in(k):
        return pltpu.make_async_copy(act.at[0, k * kc:(k + 1) * kc, 0:GB], rb.at[3, k * kc:(k + 1) * kc], fsem.at[k])

    def tile_in(s, q):
        return pltpu.make_async_copy(act.at[s // nj, :, col(s)], rb.at[q], rsem.at[q])

    def tile_out(s, q):
        return pltpu.make_async_copy(ob.at[q], dwl.at[0, s // nj, :, col(s)], osem.at[q])

    def side_in(u):
        q = u % 2
        r = pl.ds(pl.multiple_of(u * (D // ns), 16), D // ns)
        t = pl.ds(pl.multiple_of(u * (KY * RC // ns), 16), KY * RC // ns)
        return (pltpu.make_async_copy(dxi.at[r, :], dv.at[q], dsem.at[0, q]),
                pltpu.make_async_copy(gs.at[t, :], gv.at[q, 0], gsem.at[q, 0]),
                pltpu.make_async_copy(ys.at[t, :], gv.at[q, 1], gsem.at[q, 1]))

    def side_out(u):
        q = u % 2
        r = pl.ds(pl.multiple_of(u * (D // ns), 16), D // ns)
        t = pl.ds(pl.multiple_of(u * (KY * RC // ns), 16), KY * RC // ns)
        return (pltpu.make_async_copy(dv.at[q], dxo.at[r, :], dsem.at[1, q]),
                pltpu.make_async_copy(sv.at[q], dwn.at[t, :], ssem.at[q]))

    dy_in = pltpu.make_async_copy(dy, lhs.at[1], ysem)
    for k in range(nk):
        x_in(k).start()
        first_in(k).start()
    for t in (0, 1):
        tile_in(1 + t, t).start()
    dy_in.start()
    for k in range(nk):
        x_in(k).wait()
        first_in(k).wait()
        part = jnp.dot(lhs[0, :, k * kc:(k + 1) * kc], rb[3, k * kc:(k + 1) * kc], preferred_element_type=F32)
        ob[1] = part if k == 0 else ob[1] + part
    tile_out(0, 1).start()

    @pl.loop(0, ni)
    def _(u):
        s = 1 + 2 * u
        b = u % 2 * 2

        @pl.when(u < ni - 1)
        def _():
            for t in (0, 1):
                tile_in(s + 2 + t, 2 - b + t).start()

        @pl.when(u >= 2)
        def _():
            for cp in side_out(u - 2):
                cp.wait()

        @pl.when(u < ns)
        def _():
            for cp in side_in(u):
                cp.start()

        @pl.when(u >= 1)
        def _():
            for cp in side_in(u - 1):
                cp.wait()
            tile_out(s, 0).wait()

        @pl.when(u == 4)
        def _():
            dy_in.wait()

        for t in (0, 1):
            tile_in(s + t, b + t).wait()
        tile_out(s, 1).wait()
        for t in (0, 1):
            ob[t] = jnp.dot(lhs[(s + t) // (2 * nj)], rb[b + t], preferred_element_type=F32)
            if t == 0:
                sv[1 - u % 2] = gv[1 - u % 2, 0].astype(F32) + gv[1 - u % 2, 1].astype(F32)
            tile_out(s + t, t).start()

        @pl.when(u >= 1)
        def _():
            for cp in side_out(u - 1):
                cp.start()

    for cp in side_out(ns - 1):
        cp.wait()
    for t in (0, 1):
        tile_out(t, t).wait()


def gw_call(xT, dyT, act, dxi, gs, ys):
    V, kr = pltpu.VMEM, KY * RC // 6
    return pl.pallas_call(
        gw_kernel,
        out_shape=(jax.ShapeDtypeStruct((1, 3, D, FF), F32), jax.ShapeDtypeStruct((D, T), BF),
                   jax.ShapeDtypeStruct((3 * D, SH), F32)),
        in_specs=[ANY] * 6,
        out_specs=(ANY,) * 3,
        scratch_shapes=[V((2, D, T), BF), V((4, T, GB), BF), V((2, D, GB), F32), V((2, D // 6, T), BF),
                        V((2, 2, kr, SH), BF), V((2, kr, SH), F32),
                        DMA((4,)), DMA((4,)), DMA, DMA((4,)), DMA((2,)), DMA((2, 2)), DMA((2, 2)), DMA((2,))],
        compiler_params=pltpu.CompilerParams(vmem_limit_bytes=VM),
        cost_estimate=pl.CostEstimate(flops=6 * T * D * FF, bytes_accessed=4 * T * D + 6 * T * FF + 12 * D * FF,
                                      transcendentals=0),
    )(xT, dyT, act, dxi, gs, ys)


def final_kernel(g_ref, y_ref, _, o_ref):
    o_ref[...] = g_ref[...].astype(F32) + y_ref[...].astype(F32)


def final_call(gt, yt, acc):
    rb, first = 480, KY * RC // 480
    spec = pl.BlockSpec((rb, SH), lambda i: (i, 0))
    return pl.pallas_call(
        final_kernel,
        out_shape=jax.ShapeDtypeStruct((3 * D, SH), F32),
        grid=((NK - KY) * RC // rb,), in_specs=[spec, spec, ANY],
        out_specs=pl.BlockSpec((rb, SH), lambda i: (i + first, 0)),
        input_output_aliases={2: 0},
        compiler_params=pltpu.CompilerParams(vmem_limit_bytes=VM),
        cost_estimate=pl.CostEstimate(flops=D * SH, bytes_accessed=8 * D * SH, transcendentals=0),
    )(gt, yt, acc)


def solution(mesh):
    grp = ("fo", "fi")
    alla = ("dp", "fo", "fi")
    flip = [(0, 1), (1, 0)]

    def local(x, dy, w1s, w3s, w2s, g):
        xT, dyT = x.T, dy.T
        act, _, dxT, _, _, gs, gt, ys = main_call(xT, dyT, w1s, w3s, w2s.T, g.reshape(3 * D, FF))
        yt = lax.ppermute(gt, "dp", flip)
        dwl, dxT, dwn = gw_call(xT, dyT, act, dxT, gs, ys)
        yt, dwn = lax.optimization_barrier((yt, dwn))
        dwn = final_call(gt, yt, dwn).reshape(3, D, SH)
        return dxT.T, dwn, dwl

    return jax.shard_map(
        local, mesh=mesh,
        in_specs=(P(alla, None), P(alla, None), P(None, grp), P(None, grp), P(grp, None),
                  P(alla, None, None, None)),
        out_specs=(P(alla, None), P(None, None, grp), P(alla, None, None, None)),
        check_vma=False)
```

```python
import jax
import jax.numpy as jnp
from jax import lax
from jax.experimental import pallas as pl
from jax.experimental.pallas import tpu as pltpu
from jax.sharding import PartitionSpec as P

BF = jnp.bfloat16
F32 = jnp.float32
T, D, FF = 4096, 960, 2560
SH = FF // 4
HB = FF // 2
TB = 512
NT = T // TB
NB = 256
RC = 240
NK = 3 * D // RC
DH = D // 2
KY = 8
GB = 512
VM = 63 * 1024 * 1024
ANY = pl.BlockSpec(memory_space=pl.ANY)
DMA = pltpu.SemaphoreType.DMA


def rcopy(src, dst, ss, rs, dev):
    return pltpu.make_async_remote_copy(src_ref=src, dst_ref=dst, send_sem=ss, recv_sem=rs,
                                        device_id=dev, device_id_type=pl.DeviceIdType.MESH)


def main_kernel(x, dy, w1s, w3s, w2s, g,
                act, dxp, dx, rn, ra, gs, gt, ys,
                wo, wn, xb, yb, xt, yt, hb, dab, dbb, pb, ob, xs, xr, nb, ab, gb,
                wl, wcs, wcr, wxs, wxr, wys, wyr, w1fs, w1fr, w2fs, w2fr,
                gns, gnr, gas, gar, xss, xsr, yss, ysr, ldn, lda, gst, xsem, hsem, psem, osem):
    d, o, c = lax.axis_index("dp"), lax.axis_index("fo"), lax.axis_index("fi")
    cdev, xdev, ydev = (d, o, 1 - c), (d, 1 - o, c), (1 - d, o, c)
    shards = (w1s, w3s, w2s)

    mine, other = slice(0, SH), slice(SH, HB)

    def gcols(oo, cc):
        return pl.ds(pl.multiple_of((oo * 2 + cc) * SH, 128), SH)

    def rows(k):
        return pl.ds(pl.multiple_of(k * RC, 16), RC)

    def half(dd):
        return pl.ds(pl.multiple_of(dd * DH, 16), DH)

    bar = pltpu.get_barrier_semaphore()
    for dev in (cdev, xdev, ydev):
        pl.semaphore_signal(bar, inc=1, device_id=dev, device_id_type=pl.DeviceIdType.MESH)
    pl.semaphore_wait(bar, 3)

    def c_own(m):
        return rcopy(shards[m], wo.at[m, :, other], wcs.at[m], wcr.at[m], cdev)

    def x_own(m):
        return rcopy(shards[m].at[half(d), :], wn.at[m, half(d), mine], wxs.at[m], wxr.at[m], xdev)

    def y_fwd(m):
        v = wn.at[m, half(d), mine]
        return rcopy(v, v, wys.at[m], wyr.at[m], ydev)

    def c_fwd1(m):
        return rcopy(wn.at[m, half(d), mine], wn.at[m, half(d), other], w1fs.at[m], w1fr.at[m], cdev)

    def c_fwd2(m):
        return rcopy(wn.at[m, half(1 - d), mine], wn.at[m, half(1 - d), other], w2fs.at[m], w2fr.at[m], cdev)

    def l_own(m):
        return pltpu.make_async_copy(shards[m], wo.at[m, :, mine], wl.at[m])

    def g_n(k):
        return rcopy(g.at[rows(k), gcols(1 - o, 1 - c)], rn.at[rows(k), :], gns.at[k], gnr.at[k], cdev)

    def g_a(k):
        return rcopy(g.at[rows(k), gcols(o, 1 - c)], ra.at[rows(k), :], gas.at[k], gar.at[k], cdev)

    def x_sum(k):
        return rcopy(xs.at[k], xr.at[k], xss.at[k], xsr.at[k], xdev)

    def loads(k, oo, rec, buf, sem):
        q = k % 2
        return (pltpu.make_async_copy(g.at[rows(k), gcols(oo, c)], buf.at[q, 0], sem.at[q, 0]),
                pltpu.make_async_copy(rec.at[rows(k), :], buf.at[q, 1], sem.at[q, 1]))

    def load_n(k):
        return loads(k, 1 - o, rn, nb, ldn)

    def load_a(k):
        return loads(k, o, ra, ab, lda)

    def start_n(k):
        g_n(k).wait_recv()
        for cp in load_n(k):
            cp.start()

    def start_a(k):
        g_a(k).wait_recv()
        for cp in load_a(k):
            cp.start()

    def g_out(k):
        return pltpu.make_async_copy(gb.at[k], gs.at[rows(k), :], gst.at[k])

    def t_out(k):
        return pltpu.make_async_copy(gb.at[k], gt.at[rows(k - KY), :], gst.at[k])

    def y_sum(k):
        return rcopy(gb.at[k], ys.at[rows(k), :], yss.at[k], ysr.at[k], ydev)

    def pair_sum(buf, q):
        return buf[q, 0].astype(BF) + buf[q, 1].astype(BF)

    def sum1(k, q):
        xs[k] = pair_sum(nb, q)

    def wait_a(k):
        for cp in load_a(k):
            cp.wait()
        x_sum(k).wait_recv()

    def sum2(k, q):
        gb[k] = pair_sum(ab, q) + xr[k]

    def share(k):
        g_out(k).start()
        y_sum(k).start()

    def tiles(j):
        q = j % 2
        t = pl.ds(pl.multiple_of((j % NT) * TB, 128), TB)
        return (pltpu.make_async_copy(x.at[:, t], xb.at[q], xsem.at[q, 0]),
                pltpu.make_async_copy(dy.at[:, t], yb.at[q], xsem.at[q, 1]))

    def acts(p, i):
        q = i % 2
        t = pl.ds(pl.multiple_of(i * TB, 128), TB)
        oo = o if p == 0 else 1 - o
        return [pltpu.make_async_copy(v.at[q, :, loc], act.at[m, t, gcols(oo, cc)], hsem.at[q, m, k])
                for m, v in enumerate((dab, dbb, hb)) for k, (loc, cc) in enumerate(((mine, c), (other, 1 - c)))]

    def tok(i):
        return pl.ds(pl.multiple_of(i * TB, 128), TB)

    def p_out(i):
        return pltpu.make_async_copy(pb.at[i % 2], dxp.at[:, tok(i)], psem.at[0, i % 2])

    def p_in(i):
        return pltpu.make_async_copy(dxp.at[:, tok(i)], pb.at[i % 2], psem.at[1, i % 2])

    def d_out(i):
        return pltpu.make_async_copy(ob.at[i % 2], dx.at[:, tok(i)], osem.at[i % 2])

    def transpose(q):
        xt[...] = xb[q].T
        yt[...] = yb[q].T

    for m in range(3):
        c_own(m).start()
        l_own(m).start()
    for m in range(3):
        x_own(m).start()
    for t in (0, 1):
        for cp in tiles(t):
            cp.start()
    for cp in tiles(0):
        cp.wait()
    transpose(0)
    for m in range(3):
        l_own(m).wait()

    def shard_in():
        for m in range(3):
            c_own(m).wait_recv()

        @pl.loop(0, NK)
        def _(k):
            g_n(k).start()

        @pl.loop(0, NK)
        def _(k):
            g_a(k).start()

    def step(p, i):
        j = p * NT + i
        q = i % 2
        w = (wo, wn)[p]

        def next_tile():
            for cp in tiles(j + 1):
                cp.wait()

        def start_tile():
            for cp in tiles(j + 2):
                cp.start()

        def free():
            for cp in acts(p, i):
                cp.wait()

        def wait_n():
            for cp in load_n(j - 2):
                cp.wait()

        if p == 0:
            next_tile()
            start_tile()
            for m, (s1, s2) in enumerate(((2, 5), (4, 7), (5, 8))):
                @pl.when(j == s1)
                def _():
                    x_own(m).wait_recv()
                    y_fwd(m).start()
                    c_fwd1(m).start()

                if s2 < 8:
                    @pl.when(j == s2)
                    def _():
                        y_fwd(m).wait_recv()
                        c_fwd2(m).start()

            @pl.when(i >= 2)
            def _():
                free()
                p_out(i - 2).wait()
                wait_n()

            @pl.when(i >= 1)
            def _():
                start_n(j - 1)

            @pl.when(i >= 5)
            def _():
                start_a(j - 5)

            @pl.when(i >= 6)
            def _():
                wait_a(j - 6)
                sum2(j - 6, q)
                share(j - 6)
        else:
            pl.when(i < NT - 1)(next_tile)
            pl.when(i < NT - 2)(start_tile)
            free()
            p_in(i).wait()

            @pl.when(i < NT - 1)
            def _():
                p_in(i + 1).start()

            @pl.when(i >= 2)
            def _():
                d_out(i - 2).wait()

            pl.when(i < NK + 2 - NT)(wait_n)

            @pl.when(i < NK + 1 - NT)
            def _():
                start_n(j - 1)

            start_a(j - 5)
            wait_a(j - 6)

        for n in range(HB // NB):
            if p == 0 and n == 2:
                pl.when(j == 0)(shard_in)
            cs = slice(n * NB, (n + 1) * NB)
            a = jnp.dot(xt[...], w[0, :, cs], preferred_element_type=F32)
            b = jnp.dot(xt[...], w[1, :, cs], preferred_element_type=F32)
            dh = jnp.dot(yt[...], w[2, :, cs], preferred_element_type=F32)
            s = jax.nn.sigmoid(a)
            sa = a * s
            hb[q, :, cs] = (sa * b).astype(BF)
            dab[q, :, cs] = (dh * b * (s * (1.0 + a * (1.0 - s)))).astype(BF)
            dbb[q, :, cs] = (dh * sa).astype(BF)

        def nt(m, v):
            return lax.dot_general(w[m], v[q], (((1,), (1,)), ((), ())), preferred_element_type=F32)

        transpose(1 - q)
        sum1((j + NK) % (NK + 2), q)
        if p == 0:
            pb[q] = nt(0, dab) + nt(1, dbb)
            p_out(i).start()
        else:
            sum2(j - 6, q)
            ob[q] = (pb[q] + nt(0, dab) + nt(1, dbb)).astype(BF)
            d_out(i).start()
        for cp in acts(p, i):
            cp.start()
        if p == 0:
            @pl.when(i >= 2)
            def _():
                x_sum(j - 2).start()
        else:
            @pl.when(i < NK + 2 - NT)
            def _():
                x_sum(j - 2).start()

            @pl.when(j - 6 < KY)
            def _():
                share(j - 6)

            @pl.when(j - 6 >= KY)
            def _():
                t_out(j - 6).start()

    @pl.loop(0, NT)
    def _(i):
        step(0, i)

    for i in (NT - 2, NT - 1):
        p_out(i).wait()
    p_in(0).start()
    y_fwd(2).wait_recv()
    c_fwd2(2).start()
    for m in range(3):
        c_fwd1(m).wait_recv()
        c_fwd2(m).wait_recv()

    @pl.loop(0, NT)
    def _(i):
        step(1, i)

    start_a(NK - 1)
    for k in (NK - 2, NK - 1):
        wait_a(k)
        sum2(k, k % 2)
        t_out(k).start()
    for i in (NT - 2, NT - 1):
        d_out(i).wait()
        for cp in acts(1, i):
            cp.wait()
    for m in range(3):
        for f in (c_own, x_own, y_fwd, c_fwd1, c_fwd2):
            f(m).wait_send()

    @pl.loop(0, NK)
    def _(k):
        g_n(k).wait_send()
        g_a(k).wait_send()
        x_sum(k).wait_send()

    @pl.loop(0, KY)
    def _(k):
        g_out(k).wait()
        y_sum(k).wait()

    for k in range(KY, NK):
        t_out(k).wait()


def main_call(xT, dyT, w1s, w3s, w2sT, g2):
    def out(n, m, t=BF):
        return jax.ShapeDtypeStruct((n, m), t)

    V = pltpu.VMEM
    return pl.pallas_call(
        main_kernel,
        out_shape=(jax.ShapeDtypeStruct((3, T, FF), BF), out(D, T, F32), out(D, T),
                   out(3 * D, SH, F32), out(3 * D, SH, F32),
                   out(KY * RC, SH), out((NK - KY) * RC, SH), out(KY * RC, SH)),
        in_specs=[ANY] * 6,
        out_specs=(ANY,) * 8,
        scratch_shapes=[
            V((3, D, HB), BF), V((3, D, HB), BF),
            V((2, D, TB), BF), V((2, D, TB), BF), V((TB, D), BF), V((TB, D), BF),
            V((2, TB, HB), BF), V((2, TB, HB), BF), V((2, TB, HB), BF),
            V((2, D, TB), F32), V((2, D, TB), BF),
            V((NK + 2, RC, SH), BF), V((NK, RC, SH), BF),
            V((2, 2, RC, SH), F32), V((2, 2, RC, SH), F32), V((NK, RC, SH), BF),
        ] + [DMA((3,))] * 11 + [DMA((NK,))] * 6 + [DMA((KY,))] * 2
        + [DMA((2, 2)), DMA((2, 2)), DMA((NK,)), DMA((2, 2)), DMA((2, 3, 2)), DMA((2, 2)), DMA((2,))],
        compiler_params=pltpu.CompilerParams(vmem_limit_bytes=VM, collective_id=0, has_side_effects=True),
        cost_estimate=pl.CostEstimate(flops=10 * T * D * FF, bytes_accessed=200_000_000, transcendentals=T * FF),
    )(xT, dyT, w1s, w3s, w2sT, g2)


def gw_kernel(x, dy, act, dxi, gs, ys, dwl, dxo, dwn, lhs, rb, ob, dv, gv, sv, xsem, fsem, ysem, rsem, osem, dsem, gsem, ssem):
    nj, nk, ni, ns = FF // GB, 4, 7, 6
    kc = T // nk

    def col(s):
        return pl.ds(pl.multiple_of(s % nj * GB, 128), GB)

    def x_in(k):
        return pltpu.make_async_copy(x.at[:, k * kc:(k + 1) * kc], lhs.at[0, :, k * kc:(k + 1) * kc], xsem.at[k])

    def first_in(k):
        return pltpu.make_async_copy(act.at[0, k * kc:(k + 1) * kc, 0:GB], rb.at[3, k * kc:(k + 1) * kc], fsem.at[k])

    def tile_in(s, q):
        return pltpu.make_async_copy(act.at[s // nj, :, col(s)], rb.at[q], rsem.at[q])

    def tile_out(s, q):
        return pltpu.make_async_copy(ob.at[q], dwl.at[0, s // nj, :, col(s)], osem.at[q])

    def side_in(u):
        q = u % 2
        r = pl.ds(pl.multiple_of(u * (D // ns), 16), D // ns)
        t = pl.ds(pl.multiple_of(u * (KY * RC // ns), 16), KY * RC // ns)
        return (pltpu.make_async_copy(dxi.at[r, :], dv.at[q], dsem.at[0, q]),
                pltpu.make_async_copy(gs.at[t, :], gv.at[q, 0], gsem.at[q, 0]),
                pltpu.make_async_copy(ys.at[t, :], gv.at[q, 1], gsem.at[q, 1]))

    def dx_out(u):
        r = pl.ds(pl.multiple_of(u * (D // ns), 16), D // ns)
        return pltpu.make_async_copy(dv.at[u % 2], dxo.at[r, :], dsem.at[1, u % 2])

    def n_out(u):
        t = pl.ds(pl.multiple_of(u * (KY * RC // ns), 16), KY * RC // ns)
        return pltpu.make_async_copy(sv.at[u % 2], dwn.at[t, :], ssem.at[u % 2])

    dy_in = pltpu.make_async_copy(dy, lhs.at[1], ysem)
    for k in range(nk):
        x_in(k).start()
        first_in(k).start()
    for t in (0, 1):
        tile_in(1 + t, t).start()
    dy_in.start()
    for k in range(nk):
        x_in(k).wait()
        first_in(k).wait()
        part = jnp.dot(lhs[0, :, k * kc:(k + 1) * kc], rb[3, k * kc:(k + 1) * kc], preferred_element_type=F32)
        ob[3] = part if k == 0 else ob[3] + part
    tile_out(0, 3).start()

    @pl.loop(0, ni)
    def _(u):
        s = 1 + 2 * u
        b = u % 2 * 2

        @pl.when(u < ni - 1)
        def _():
            for t in (0, 1):
                tile_in(s + 2 + t, 2 - b + t).start()

        @pl.when(u >= 2)
        def _():
            dx_out(u - 2).wait()
            tile_out(s, b).wait()

        @pl.when(u >= 3)
        def _():
            n_out(u - 3).wait()

        @pl.when(u >= 1)
        def _():
            tile_out(s, b + 1).wait()

        @pl.when(u < ns)
        def _():
            for cp in side_in(u):
                cp.start()

        @pl.when(u >= 1)
        def _():
            for cp in side_in(u - 1):
                cp.wait()
            dx_out(u - 1).start()

        @pl.when(u == 4)
        def _():
            dy_in.wait()

        for t in (0, 1):
            tile_in(s + t, b + t).wait()
        for t in (0, 1):
            ob[b + t] = jnp.dot(lhs[(s + t) // (2 * nj)], rb[b + t], preferred_element_type=F32)
            if t == 0:
                sv[1 - u % 2] = gv[1 - u % 2, 0].astype(F32) + gv[1 - u % 2, 1].astype(F32)
            tile_out(s + t, b + t).start()

        @pl.when(u >= 1)
        def _():
            n_out(u - 1).start()

    dx_out(ns - 1).wait()
    for k in (ns - 2, ns - 1):
        n_out(k).wait()
    for t in range(4):
        tile_out(t, t).wait()


def gw_call(xT, dyT, act, dxi, gs, ys):
    V, kr = pltpu.VMEM, KY * RC // 6
    return pl.pallas_call(
        gw_kernel,
        out_shape=(jax.ShapeDtypeStruct((1, 3, D, FF), F32), jax.ShapeDtypeStruct((D, T), BF),
                   jax.ShapeDtypeStruct((3 * D, SH), F32)),
        in_specs=[ANY] * 6,
        out_specs=(ANY,) * 3,
        scratch_shapes=[V((2, D, T), BF), V((4, T, GB), BF), V((4, D, GB), F32), V((2, D // 6, T), BF),
                        V((2, 2, kr, SH), BF), V((2, kr, SH), F32),
                        DMA((4,)), DMA((4,)), DMA, DMA((4,)), DMA((4,)), DMA((2, 2)), DMA((2, 2)), DMA((2,))],
        compiler_params=pltpu.CompilerParams(vmem_limit_bytes=VM),
        cost_estimate=pl.CostEstimate(flops=6 * T * D * FF, bytes_accessed=4 * T * D + 6 * T * FF + 12 * D * FF,
                                      transcendentals=0),
    )(xT, dyT, act, dxi, gs, ys)


def final_kernel(g_ref, y_ref, _, o_ref):
    o_ref[...] = g_ref[...].astype(F32) + y_ref[...].astype(F32)


def final_call(gt, yt, acc):
    rb, first = 480, KY * RC // 480
    spec = pl.BlockSpec((rb, SH), lambda i: (i, 0))
    return pl.pallas_call(
        final_kernel,
        out_shape=jax.ShapeDtypeStruct((3 * D, SH), F32),
        grid=((NK - KY) * RC // rb,), in_specs=[spec, spec, ANY],
        out_specs=pl.BlockSpec((rb, SH), lambda i: (i + first, 0)),
        input_output_aliases={2: 0},
        compiler_params=pltpu.CompilerParams(vmem_limit_bytes=VM),
        cost_estimate=pl.CostEstimate(flops=D * SH, bytes_accessed=8 * D * SH, transcendentals=0),
    )(gt, yt, acc)


def solution(mesh):
    grp = ("fo", "fi")
    alla = ("dp", "fo", "fi")
    flip = [(0, 1), (1, 0)]

    def local(x, dy, w1s, w3s, w2s, g):
        xT, dyT = x.T, dy.T
        act, _, dxT, _, _, gs, gt, ys = main_call(xT, dyT, w1s, w3s, w2s.T, g.reshape(3 * D, FF))
        yt = lax.ppermute(gt, "dp", flip)
        dwl, dxT, dwn = gw_call(xT, dyT, act, dxT, gs, ys)
        yt, dwn = lax.optimization_barrier((yt, dwn))
        dwn = final_call(gt, yt, dwn).reshape(3, D, SH)
        return dxT.T, dwn, dwl

    return jax.shard_map(
        local, mesh=mesh,
        in_specs=(P(alla, None), P(alla, None), P(None, grp), P(None, grp), P(grp, None),
                  P(alla, None, None, None)),
        out_specs=(P(alla, None), P(None, None, grp), P(alla, None, None, None)),
        check_vma=False)
```

```python
import jax
import jax.numpy as jnp
from jax import lax
from jax.experimental import pallas as pl
from jax.experimental.pallas import tpu as pltpu
from jax.sharding import PartitionSpec as P

BF = jnp.bfloat16
F32 = jnp.float32
T, D, FF = 4096, 960, 2560
SH = FF // 4
HB = FF // 2
TB = 512
NT = T // TB
NB = 256
RC = 240
NK = 3 * D // RC
DH = D // 2
KY = 8
GB = 512
VM = 63 * 1024 * 1024
ANY = pl.BlockSpec(memory_space=pl.ANY)
DMA = pltpu.SemaphoreType.DMA


def rcopy(src, dst, ss, rs, dev):
    return pltpu.make_async_remote_copy(src_ref=src, dst_ref=dst, send_sem=ss, recv_sem=rs,
                                        device_id=dev, device_id_type=pl.DeviceIdType.MESH)


def main_kernel(x, dy, w1s, w3s, w2s, g,
                act, dxp, dx, rn, ra, gs, gt, ys,
                wo, wn, xb, yb, xt, yt, hb, dab, dbb, pb, ob, xs, xr, nb, ab, gb,
                wl, wcs, wcr, wxs, wxr, wys, wyr, w1fs, w1fr, w2fs, w2fr,
                gns, gnr, gas, gar, xss, xsr, yss, ysr, ldn, lda, gst, xsem, hsem, psem, osem):
    d, o, c = lax.axis_index("dp"), lax.axis_index("fo"), lax.axis_index("fi")
    cdev, xdev, ydev = (d, o, 1 - c), (d, 1 - o, c), (1 - d, o, c)
    shards = (w1s, w3s, w2s)

    mine, other = slice(0, SH), slice(SH, HB)

    def gcols(oo, cc):
        return pl.ds(pl.multiple_of((oo * 2 + cc) * SH, 128), SH)

    def rows(k):
        return pl.ds(pl.multiple_of(k * RC, 16), RC)

    def half(dd):
        return pl.ds(pl.multiple_of(dd * DH, 16), DH)

    bar = pltpu.get_barrier_semaphore()
    for dev in (cdev, xdev, ydev):
        pl.semaphore_signal(bar, inc=1, device_id=dev, device_id_type=pl.DeviceIdType.MESH)
    pl.semaphore_wait(bar, 3)

    def c_own(m):
        return rcopy(shards[m], wo.at[m, :, other], wcs.at[m], wcr.at[m], cdev)

    def x_own(m):
        return rcopy(shards[m].at[half(d), :], wn.at[m, half(d), mine], wxs.at[m], wxr.at[m], xdev)

    def y_fwd(m):
        v = wn.at[m, half(d), mine]
        return rcopy(v, v, wys.at[m], wyr.at[m], ydev)

    def c_fwd1(m):
        return rcopy(wn.at[m, half(d), mine], wn.at[m, half(d), other], w1fs.at[m], w1fr.at[m], cdev)

    def c_fwd2(m):
        return rcopy(wn.at[m, half(1 - d), mine], wn.at[m, half(1 - d), other], w2fs.at[m], w2fr.at[m], cdev)

    def l_own(m):
        return pltpu.make_async_copy(shards[m], wo.at[m, :, mine], wl.at[m])

    def g_n(k):
        return rcopy(g.at[rows(k), gcols(1 - o, 1 - c)], rn.at[rows(k), :], gns.at[k], gnr.at[k], cdev)

    def g_a(k):
        return rcopy(g.at[rows(k), gcols(o, 1 - c)], ra.at[rows(k), :], gas.at[k], gar.at[k], cdev)

    def x_sum(k):
        return rcopy(xs.at[k], xr.at[k], xss.at[k], xsr.at[k], xdev)

    def loads(k, q, oo, rec, buf, sem):
        return (pltpu.make_async_copy(g.at[rows(k), gcols(oo, c)], buf.at[q, 0], sem.at[q, 0]),
                pltpu.make_async_copy(rec.at[rows(k), :], buf.at[q, 1], sem.at[q, 1]))

    def load_n(k):
        return loads(k, k % 2, 1 - o, rn, nb, ldn)

    def load_a(k):
        return loads(k, k % 4, o, ra, ab, lda)

    def start_n(k):
        g_n(k).wait_recv()
        for cp in load_n(k):
            cp.start()

    def start_a(k):
        g_a(k).wait_recv()
        for cp in load_a(k):
            cp.start()

    def g_out(k):
        return pltpu.make_async_copy(gb.at[k], gs.at[rows(k), :], gst.at[k])

    def t_out(k):
        return pltpu.make_async_copy(gb.at[k], gt.at[rows(k - KY), :], gst.at[k])

    def y_sum(k):
        return rcopy(gb.at[k], ys.at[rows(k), :], yss.at[k], ysr.at[k], ydev)

    def pair_sum(buf, q):
        return buf[q, 0].astype(BF) + buf[q, 1].astype(BF)

    def sum1(k, q):
        xs[k] = pair_sum(nb, q)

    def wait_a(k):
        for cp in load_a(k):
            cp.wait()
        x_sum(k).wait_recv()

    def sum2(k):
        gb[k] = pair_sum(ab, k % 4) + xr[k]

    def share(k):
        g_out(k).start()
        y_sum(k).start()

    def tiles(j):
        q = j % 2
        t = pl.ds(pl.multiple_of((j % NT) * TB, 128), TB)
        return (pltpu.make_async_copy(x.at[:, t], xb.at[q], xsem.at[q, 0]),
                pltpu.make_async_copy(dy.at[:, t], yb.at[q], xsem.at[q, 1]))

    def acts(p, i):
        q = i % 2
        t = pl.ds(pl.multiple_of(i * TB, 128), TB)
        oo = o if p == 0 else 1 - o
        return [pltpu.make_async_copy(v.at[q, :, loc], act.at[m, t, gcols(oo, cc)], hsem.at[q, m, k])
                for m, v in enumerate((dab, dbb, hb)) for k, (loc, cc) in enumerate(((mine, c), (other, 1 - c)))]

    def tok(i):
        return pl.ds(pl.multiple_of(i * TB, 128), TB)

    def p_out(i):
        return pltpu.make_async_copy(pb.at[i % 2], dxp.at[:, tok(i)], psem.at[0, i % 2])

    def p_in(i):
        return pltpu.make_async_copy(dxp.at[:, tok(i)], pb.at[i % 2], psem.at[1, i % 2])

    def d_out(i):
        return pltpu.make_async_copy(ob.at[i % 2], dx.at[:, tok(i)], osem.at[i % 2])

    def transpose(q):
        xt[...] = xb[q].T
        yt[...] = yb[q].T

    for m in range(3):
        c_own(m).start()
        l_own(m).start()
    for m in range(3):
        x_own(m).start()
    for t in (0, 1):
        for cp in tiles(t):
            cp.start()
    for cp in tiles(0):
        cp.wait()
    transpose(0)
    for m in range(3):
        l_own(m).wait()

    def shard_in():
        for m in range(3):
            c_own(m).wait_recv()

        @pl.loop(0, NK)
        def _(k):
            g_n(k).start()

        @pl.loop(0, NK)
        def _(k):
            g_a(k).start()

    def step(p, i):
        j = p * NT + i
        q = i % 2
        w = (wo, wn)[p]

        def next_tile():
            for cp in tiles(j + 1):
                cp.wait()

        def start_tile():
            for cp in tiles(j + 2):
                cp.start()

        def free():
            for cp in acts(p, i):
                cp.wait()

        def wait_n():
            for cp in load_n(j - 2):
                cp.wait()

        if p == 0:
            next_tile()
            start_tile()
            for m, (s1, s2) in enumerate(((2, 5), (4, 7), (6, 8))):
                @pl.when(j == s1)
                def _():
                    x_own(m).wait_recv()
                    y_fwd(m).start()
                    c_fwd1(m).start()

                if s2 < 8:
                    @pl.when(j == s2)
                    def _():
                        y_fwd(m).wait_recv()
                        c_fwd2(m).start()

            @pl.when(i >= 2)
            def _():
                free()
                p_out(i - 2).wait()
                wait_n()

            @pl.when(i >= 1)
            def _():
                start_n(j - 1)

            @pl.when(i >= 5)
            def _():
                start_a(j - 5)

            @pl.when(i >= 6)
            def _():
                wait_a(j - 6)
                sum2(j - 6)
                share(j - 6)
        else:
            pl.when(i < NT - 1)(next_tile)
            pl.when(i < NT - 2)(start_tile)
            free()
            p_in(i).wait()

            @pl.when(i < NT - 1)
            def _():
                p_in(i + 1).start()

            @pl.when(i >= 2)
            def _():
                d_out(i - 2).wait()

            pl.when(i < NK + 2 - NT)(wait_n)

            @pl.when(i < NK + 1 - NT)
            def _():
                start_n(j - 1)

            start_a(j - 5)
            pl.when(i == NT - 1)(lambda: start_a(NK - 1))
            wait_a(j - 6)

        for n in range(HB // NB):
            if p == 0 and n == 2:
                pl.when(j == 0)(shard_in)
            cs = slice(n * NB, (n + 1) * NB)
            a = jnp.dot(xt[...], w[0, :, cs], preferred_element_type=F32)
            b = jnp.dot(xt[...], w[1, :, cs], preferred_element_type=F32)
            dh = jnp.dot(yt[...], w[2, :, cs], preferred_element_type=F32)
            s = jax.nn.sigmoid(a)
            sa = a * s
            hb[q, :, cs] = (sa * b).astype(BF)
            dab[q, :, cs] = (dh * b * (s * (1.0 + a * (1.0 - s)))).astype(BF)
            dbb[q, :, cs] = (dh * sa).astype(BF)

        def nt(m, v):
            return lax.dot_general(w[m], v[q], (((1,), (1,)), ((), ())), preferred_element_type=F32)

        transpose(1 - q)
        sum1((j + NK) % (NK + 2), q)
        if p == 0:
            pb[q] = nt(0, dab) + nt(1, dbb)
            p_out(i).start()
        else:
            sum2(j - 6)
            ob[q] = (pb[q] + nt(0, dab) + nt(1, dbb)).astype(BF)
            d_out(i).start()
        for cp in acts(p, i):
            cp.start()
        if p == 0:
            @pl.when(i >= 2)
            def _():
                x_sum(j - 2).start()

            @pl.when(i == NT - 1)
            def _():
                p_out(NT - 2).wait()
                p_in(0).start()
        else:
            @pl.when(i < NK + 2 - NT)
            def _():
                x_sum(j - 2).start()

            @pl.when(j - 6 < KY)
            def _():
                share(j - 6)

            @pl.when(j - 6 >= KY)
            def _():
                t_out(j - 6).start()

    @pl.loop(0, NT)
    def _(i):
        step(0, i)

    y_fwd(2).wait_recv()
    c_fwd2(2).start()
    p_out(NT - 1).wait()
    for m in range(3):
        c_fwd1(m).wait_recv()
        c_fwd2(m).wait_recv()

    @pl.loop(0, NT)
    def _(i):
        step(1, i)

    for k in (NK - 2, NK - 1):
        wait_a(k)
        sum2(k)
        t_out(k).start()
    for i in (NT - 2, NT - 1):
        d_out(i).wait()
        for cp in acts(1, i):
            cp.wait()
    for m in range(3):
        for f in (c_own, x_own, y_fwd, c_fwd1, c_fwd2):
            f(m).wait_send()

    @pl.loop(0, NK)
    def _(k):
        g_n(k).wait_send()
        g_a(k).wait_send()
        x_sum(k).wait_send()

    @pl.loop(0, KY)
    def _(k):
        g_out(k).wait()
        y_sum(k).wait()

    for k in range(KY, NK):
        t_out(k).wait()


def main_call(xT, dyT, w1s, w3s, w2sT, g2):
    def out(n, m, t=BF):
        return jax.ShapeDtypeStruct((n, m), t)

    V = pltpu.VMEM
    return pl.pallas_call(
        main_kernel,
        out_shape=(jax.ShapeDtypeStruct((3, T, FF), BF), out(D, T, F32), out(D, T),
                   out(3 * D, SH, F32), out(3 * D, SH, F32),
                   out(KY * RC, SH), out((NK - KY) * RC, SH), out(KY * RC, SH)),
        in_specs=[ANY] * 6,
        out_specs=(ANY,) * 8,
        scratch_shapes=[
            V((3, D, HB), BF), V((3, D, HB), BF),
            V((2, D, TB), BF), V((2, D, TB), BF), V((TB, D), BF), V((TB, D), BF),
            V((2, TB, HB), BF), V((2, TB, HB), BF), V((2, TB, HB), BF),
            V((2, D, TB), F32), V((2, D, TB), BF),
            V((NK + 2, RC, SH), BF), V((NK, RC, SH), BF),
            V((2, 2, RC, SH), F32), V((4, 2, RC, SH), F32), V((NK, RC, SH), BF),
        ] + [DMA((3,))] * 11 + [DMA((NK,))] * 6 + [DMA((KY,))] * 2
        + [DMA((2, 2)), DMA((4, 2)), DMA((NK,)), DMA((2, 2)), DMA((2, 3, 2)), DMA((2, 2)), DMA((2,))],
        compiler_params=pltpu.CompilerParams(vmem_limit_bytes=VM, collective_id=0, has_side_effects=True),
        cost_estimate=pl.CostEstimate(flops=10 * T * D * FF, bytes_accessed=200_000_000, transcendentals=T * FF),
    )(xT, dyT, w1s, w3s, w2sT, g2)


def gw_kernel(x, dy, act, dxi, gs, ys, dwl, dxo, dwn, lhs, rb, ob, dv, gv, sv, xsem, fsem, ysem, rsem, osem, dsem, gsem, ssem):
    nj, nk, ni, ns = FF // GB, 4, 7, 6
    kc = T // nk

    def col(s):
        return pl.ds(pl.multiple_of(s % nj * GB, 128), GB)

    def x_in(k):
        return pltpu.make_async_copy(x.at[:, k * kc:(k + 1) * kc], lhs.at[0, :, k * kc:(k + 1) * kc], xsem.at[k])

    def first_in(k):
        return pltpu.make_async_copy(act.at[0, k * kc:(k + 1) * kc, 0:GB], rb.at[3, k * kc:(k + 1) * kc], fsem.at[k])

    def tile_in(s, q):
        return pltpu.make_async_copy(act.at[s // nj, :, col(s)], rb.at[q], rsem.at[q])

    def tile_out(s, q):
        return pltpu.make_async_copy(ob.at[q], dwl.at[0, s // nj, :, col(s)], osem.at[q])

    def side_in(u):
        q = u % 2
        r = pl.ds(pl.multiple_of(u * (D // ns), 16), D // ns)
        t = pl.ds(pl.multiple_of(u * (KY * RC // ns), 16), KY * RC // ns)
        return (pltpu.make_async_copy(dxi.at[r, :], dv.at[q], dsem.at[0, q]),
                pltpu.make_async_copy(gs.at[t, :], gv.at[q, 0], gsem.at[q, 0]),
                pltpu.make_async_copy(ys.at[t, :], gv.at[q, 1], gsem.at[q, 1]))

    def dx_out(u):
        r = pl.ds(pl.multiple_of(u * (D // ns), 16), D // ns)
        return pltpu.make_async_copy(dv.at[u % 2], dxo.at[r, :], dsem.at[1, u % 2])

    def n_out(u):
        t = pl.ds(pl.multiple_of(u * (KY * RC // ns), 16), KY * RC // ns)
        return pltpu.make_async_copy(sv.at[u % 2], dwn.at[t, :], ssem.at[u % 2])

    dy_in = pltpu.make_async_copy(dy, lhs.at[1], ysem)
    for k in range(nk):
        x_in(k).start()
        first_in(k).start()
    for t in (0, 1):
        tile_in(1 + t, t).start()
    dy_in.start()
    for k in range(nk):
        x_in(k).wait()
        first_in(k).wait()
        part = jnp.dot(lhs[0, :, k * kc:(k + 1) * kc], rb[3, k * kc:(k + 1) * kc], preferred_element_type=F32)
        ob[3] = part if k == 0 else ob[3] + part
    tile_out(0, 3).start()

    @pl.loop(0, ni)
    def _(u):
        s = 1 + 2 * u
        b = u % 2 * 2

        @pl.when(u < ni - 1)
        def _():
            for t in (0, 1):
                tile_in(s + 2 + t, 2 - b + t).start()

        @pl.when(u >= 2)
        def _():
            dx_out(u - 2).wait()
            tile_out(s, b).wait()

        @pl.when(u >= 3)
        def _():
            n_out(u - 3).wait()

        @pl.when(u >= 1)
        def _():
            tile_out(s, b + 1).wait()

        @pl.when(u < ns)
        def _():
            for cp in side_in(u):
                cp.start()

        @pl.when(u >= 1)
        def _():
            for cp in side_in(u - 1):
                cp.wait()
            dx_out(u - 1).start()

        @pl.when(u == 4)
        def _():
            dy_in.wait()

        for t in (0, 1):
            tile_in(s + t, b + t).wait()
        for t in (0, 1):
            ob[b + t] = jnp.dot(lhs[(s + t) // (2 * nj)], rb[b + t], preferred_element_type=F32)
            if t == 0:
                sv[1 - u % 2] = gv[1 - u % 2, 0].astype(F32) + gv[1 - u % 2, 1].astype(F32)
            tile_out(s + t, b + t).start()

        @pl.when(u >= 1)
        def _():
            n_out(u - 1).start()

    dx_out(ns - 1).wait()
    for k in (ns - 2, ns - 1):
        n_out(k).wait()
    for t in range(4):
        tile_out(t, t).wait()


def gw_call(xT, dyT, act, dxi, gs, ys):
    V, kr = pltpu.VMEM, KY * RC // 6
    return pl.pallas_call(
        gw_kernel,
        out_shape=(jax.ShapeDtypeStruct((1, 3, D, FF), F32), jax.ShapeDtypeStruct((D, T), BF),
                   jax.ShapeDtypeStruct((3 * D, SH), F32)),
        in_specs=[ANY] * 6,
        out_specs=(ANY,) * 3,
        scratch_shapes=[V((2, D, T), BF), V((4, T, GB), BF), V((4, D, GB), F32), V((2, D // 6, T), BF),
                        V((2, 2, kr, SH), BF), V((2, kr, SH), F32),
                        DMA((4,)), DMA((4,)), DMA, DMA((4,)), DMA((4,)), DMA((2, 2)), DMA((2, 2)), DMA((2,))],
        compiler_params=pltpu.CompilerParams(vmem_limit_bytes=VM),
        cost_estimate=pl.CostEstimate(flops=6 * T * D * FF, bytes_accessed=4 * T * D + 6 * T * FF + 12 * D * FF,
                                      transcendentals=0),
    )(xT, dyT, act, dxi, gs, ys)


def final_kernel(g_ref, y_ref, _, o_ref):
    o_ref[...] = g_ref[...].astype(F32) + y_ref[...].astype(F32)


def final_call(gt, yt, acc):
    rb, first = RC, KY
    spec = pl.BlockSpec((rb, SH), lambda i: (i, 0))
    return pl.pallas_call(
        final_kernel,
        out_shape=jax.ShapeDtypeStruct((3 * D, SH), F32),
        grid=((NK - KY) * RC // rb,), in_specs=[spec, spec, ANY],
        out_specs=pl.BlockSpec((rb, SH), lambda i: (i + first, 0)),
        input_output_aliases={2: 0},
        compiler_params=pltpu.CompilerParams(vmem_limit_bytes=VM),
        cost_estimate=pl.CostEstimate(flops=D * SH, bytes_accessed=8 * D * SH, transcendentals=0),
    )(gt, yt, acc)


def solution(mesh):
    grp = ("fo", "fi")
    alla = ("dp", "fo", "fi")
    flip = [(0, 1), (1, 0)]

    def local(x, dy, w1s, w3s, w2s, g):
        xT, dyT = x.T, dy.T
        act, _, dxT, _, _, gs, gt, ys = main_call(xT, dyT, w1s, w3s, w2s.T, g.reshape(3 * D, FF))
        yt = lax.ppermute(gt, "dp", flip)
        dwl, dxT, dwn = gw_call(xT, dyT, act, dxT, gs, ys)
        yt, dwn = lax.optimization_barrier((yt, dwn))
        dwn = final_call(gt, yt, dwn).reshape(3, D, SH)
        return dxT.T, dwn, dwl

    return jax.shard_map(
        local, mesh=mesh,
        in_specs=(P(alla, None), P(alla, None), P(None, grp), P(None, grp), P(grp, None),
                  P(alla, None, None, None)),
        out_specs=(P(alla, None), P(None, None, grp), P(alla, None, None, None)),
        check_vma=False)
```

```python
import jax
import jax.numpy as jnp
from jax import lax
from jax.experimental import pallas as pl
from jax.experimental.pallas import tpu as pltpu
from jax.sharding import PartitionSpec as P

BF = jnp.bfloat16
F32 = jnp.float32
T, D, FF = 4096, 960, 2560
SH = FF // 4
HB = FF // 2
TB = 512
NT = T // TB
NB = 256
RC = 240
NK = 3 * D // RC
DH = D // 2
KY = 8
GB = 512
VM = 63 * 1024 * 1024
ANY = pl.BlockSpec(memory_space=pl.ANY)
DMA = pltpu.SemaphoreType.DMA


def rcopy(src, dst, ss, rs, dev):
    return pltpu.make_async_remote_copy(src_ref=src, dst_ref=dst, send_sem=ss, recv_sem=rs,
                                        device_id=dev, device_id_type=pl.DeviceIdType.MESH)


def main_kernel(x, dy, w1s, w3s, w2s, g,
                act, dxp, dx, rn, ra, gs, gt, ys,
                wo, wn, xb, yb, xt, yt, hb, dab, dbb, pb, ob, xs, xr, nb, ab, gb,
                wl, wcs, wcr, wxs, wxr, wys, wyr, w1fs, w1fr, w2fs, w2fr,
                gns, gnr, gas, gar, xss, xsr, yss, ysr, ldn, lda, gst, xsem, hsem, psem, osem):
    d, o, c = lax.axis_index("dp"), lax.axis_index("fo"), lax.axis_index("fi")
    cdev, xdev, ydev = (d, o, 1 - c), (d, 1 - o, c), (1 - d, o, c)
    shards = (w1s, w3s, w2s)

    mine, other = slice(0, SH), slice(SH, HB)

    def gcols(oo, cc):
        return pl.ds(pl.multiple_of((oo * 2 + cc) * SH, 128), SH)

    def rows(k):
        return pl.ds(pl.multiple_of(k * RC, 16), RC)

    def half(dd):
        return pl.ds(pl.multiple_of(dd * DH, 16), DH)

    bar = pltpu.get_barrier_semaphore()
    for dev in (cdev, xdev, ydev):
        pl.semaphore_signal(bar, inc=1, device_id=dev, device_id_type=pl.DeviceIdType.MESH)
    pl.semaphore_wait(bar, 3)

    def c_own(m):
        return rcopy(shards[m], wo.at[m, :, other], wcs.at[m], wcr.at[m], cdev)

    def x_own(m):
        return rcopy(shards[m].at[half(d), :], wn.at[m, half(d), mine], wxs.at[m], wxr.at[m], xdev)

    def y_fwd(m):
        v = wn.at[m, half(d), mine]
        return rcopy(v, v, wys.at[m], wyr.at[m], ydev)

    def c_fwd1(m):
        return rcopy(wn.at[m, half(d), mine], wn.at[m, half(d), other], w1fs.at[m], w1fr.at[m], cdev)

    def c_fwd2(m):
        return rcopy(wn.at[m, half(1 - d), mine], wn.at[m, half(1 - d), other], w2fs.at[m], w2fr.at[m], cdev)

    def l_own(m):
        return pltpu.make_async_copy(shards[m], wo.at[m, :, mine], wl.at[m])

    def g_n(k):
        return rcopy(g.at[rows(k), gcols(1 - o, 1 - c)], rn.at[rows(k), :], gns.at[k], gnr.at[k], cdev)

    def g_a(k):
        return rcopy(g.at[rows(k), gcols(o, 1 - c)], ra.at[rows(k), :], gas.at[k], gar.at[k], cdev)

    def x_sum(k):
        return rcopy(xs.at[k], xr.at[k], xss.at[k], xsr.at[k], xdev)

    def loads(k, q, oo, rec, buf, sem):
        return (pltpu.make_async_copy(g.at[rows(k), gcols(oo, c)], buf.at[q, 0], sem.at[q, 0]),
                pltpu.make_async_copy(rec.at[rows(k), :], buf.at[q, 1], sem.at[q, 1]))

    def load_n(k):
        return loads(k, k % 2, 1 - o, rn, nb, ldn)

    def load_a(k):
        return loads(k, k % 4, o, ra, ab, lda)

    def start_n(k):
        g_n(k).wait_recv()
        for cp in load_n(k):
            cp.start()

    def start_a(k):
        g_a(k).wait_recv()
        for cp in load_a(k):
            cp.start()

    def g_out(k):
        return pltpu.make_async_copy(gb.at[k], gs.at[rows(k), :], gst.at[k])

    def t_out(k):
        return pltpu.make_async_copy(gb.at[k], gt.at[rows(k - KY), :], gst.at[k])

    def y_sum(k):
        return rcopy(gb.at[k], ys.at[rows(k), :], yss.at[k], ysr.at[k], ydev)

    def pair_sum(buf, q):
        return buf[q, 0].astype(BF) + buf[q, 1].astype(BF)

    def sum1(k, q):
        xs[k] = pair_sum(nb, q)

    def wait_a(k):
        for cp in load_a(k):
            cp.wait()
        x_sum(k).wait_recv()

    def sum2(k):
        gb[k] = pair_sum(ab, k % 4) + xr[k]

    def share(k):
        g_out(k).start()
        y_sum(k).start()

    def tiles(j):
        q = j % 2
        t = pl.ds(pl.multiple_of((j % NT) * TB, 128), TB)
        return (pltpu.make_async_copy(x.at[:, t], xb.at[q], xsem.at[q, 0]),
                pltpu.make_async_copy(dy.at[:, t], yb.at[q], xsem.at[q, 1]))

    def acts(p, i):
        q = i % 2
        t = pl.ds(pl.multiple_of(i * TB, 128), TB)
        oo = o if p == 0 else 1 - o
        return [pltpu.make_async_copy(v.at[q, :, loc], act.at[m, t, gcols(oo, cc)], hsem.at[q, m, k])
                for m, v in enumerate((dab, dbb, hb)) for k, (loc, cc) in enumerate(((mine, c), (other, 1 - c)))]

    def tok(i):
        return pl.ds(pl.multiple_of(i * TB, 128), TB)

    def p_out(i):
        return pltpu.make_async_copy(pb.at[i % 2], dxp.at[:, tok(i)], psem.at[0, i % 2])

    def p_in(i):
        return pltpu.make_async_copy(dxp.at[:, tok(i)], pb.at[i % 2], psem.at[1, i % 2])

    def d_out(i):
        return pltpu.make_async_copy(ob.at[i % 2], dx.at[:, tok(i)], osem.at[i % 2])

    def transpose(q):
        xt[...] = xb[q].T
        yt[...] = yb[q].T

    for m in range(3):
        c_own(m).start()
        l_own(m).start()
    for m in range(3):
        x_own(m).start()
    for t in (0, 1):
        for cp in tiles(t):
            cp.start()
    for cp in tiles(0):
        cp.wait()
    transpose(0)
    for m in range(3):
        l_own(m).wait()

    def shard_in():
        for m in range(3):
            c_own(m).wait_recv()

        @pl.loop(0, NK)
        def _(k):
            g_n(k).start()

        @pl.loop(0, NK)
        def _(k):
            g_a(k).start()

    shard_in()

    def step(p, i):
        j = p * NT + i
        q = i % 2
        w = (wo, wn)[p]

        def next_tile():
            for cp in tiles(j + 1):
                cp.wait()

        def start_tile():
            for cp in tiles(j + 2):
                cp.start()

        def free():
            for cp in acts(p, i):
                cp.wait()

        def wait_n():
            for cp in load_n(j - 2):
                cp.wait()

        if p == 0:
            next_tile()
            start_tile()
            for m, (s1, s2) in enumerate(((2, 5), (4, 7), (6, 8))):
                @pl.when(j == s1)
                def _():
                    x_own(m).wait_recv()
                    y_fwd(m).start()
                    c_fwd1(m).start()

                if s2 < 8:
                    @pl.when(j == s2)
                    def _():
                        y_fwd(m).wait_recv()
                        c_fwd2(m).start()

            @pl.when(i >= 2)
            def _():
                free()
                p_out(i - 2).wait()
                wait_n()

            @pl.when(i >= 1)
            def _():
                start_n(j - 1)

            @pl.when(i >= 5)
            def _():
                start_a(j - 5)

            @pl.when(i >= 6)
            def _():
                wait_a(j - 6)
                sum2(j - 6)
                share(j - 6)
        else:
            pl.when(i < NT - 1)(next_tile)
            pl.when(i < NT - 2)(start_tile)
            free()
            p_in(i).wait()

            @pl.when(i < NT - 1)
            def _():
                p_in(i + 1).start()

            @pl.when(i >= 2)
            def _():
                d_out(i - 2).wait()

            pl.when(i < NK + 2 - NT)(wait_n)

            @pl.when(i < NK + 1 - NT)
            def _():
                start_n(j - 1)

            start_a(j - 5)
            pl.when(i == NT - 1)(lambda: start_a(NK - 1))
            wait_a(j - 6)

        for n in range(HB // NB):
            cs = slice(n * NB, (n + 1) * NB)
            a = jnp.dot(xt[...], w[0, :, cs], preferred_element_type=F32)
            b = jnp.dot(xt[...], w[1, :, cs], preferred_element_type=F32)
            dh = jnp.dot(yt[...], w[2, :, cs], preferred_element_type=F32)
            s = jax.nn.sigmoid(a)
            sa = a * s
            hb[q, :, cs] = (sa * b).astype(BF)
            dab[q, :, cs] = (dh * b * (s + sa * (1.0 - s))).astype(BF)
            dbb[q, :, cs] = (dh * sa).astype(BF)

        def nt(m, v):
            return lax.dot_general(w[m], v[q], (((1,), (1,)), ((), ())), preferred_element_type=F32)

        transpose(1 - q)
        sum1((j + NK) % (NK + 2), q)
        if p == 0:
            pb[q] = nt(0, dab) + nt(1, dbb)
            p_out(i).start()
        else:
            sum2(j - 6)
            ob[q] = (pb[q] + nt(0, dab) + nt(1, dbb)).astype(BF)
            d_out(i).start()
        for cp in acts(p, i):
            cp.start()
        if p == 0:
            @pl.when(i >= 2)
            def _():
                x_sum(j - 2).start()

            @pl.when(i == NT - 1)
            def _():
                p_out(NT - 2).wait()
                p_in(0).start()
        else:
            @pl.when(i < NK + 2 - NT)
            def _():
                x_sum(j - 2).start()

            @pl.when(j - 6 < KY)
            def _():
                share(j - 6)

            @pl.when(j - 6 >= KY)
            def _():
                t_out(j - 6).start()

    @pl.loop(0, NT)
    def _(i):
        step(0, i)

    y_fwd(2).wait_recv()
    c_fwd2(2).start()
    p_out(NT - 1).wait()
    for m in range(3):
        c_fwd1(m).wait_recv()
        c_fwd2(m).wait_recv()

    @pl.loop(0, NT)
    def _(i):
        step(1, i)

    for k in (NK - 2, NK - 1):
        wait_a(k)
        sum2(k)
        t_out(k).start()
    for i in (NT - 2, NT - 1):
        d_out(i).wait()
        for cp in acts(1, i):
            cp.wait()
    for m in range(3):
        for f in (c_own, x_own, y_fwd, c_fwd1, c_fwd2):
            f(m).wait_send()

    @pl.loop(0, NK)
    def _(k):
        g_n(k).wait_send()
        g_a(k).wait_send()
        x_sum(k).wait_send()

    @pl.loop(0, KY)
    def _(k):
        g_out(k).wait()
        y_sum(k).wait()

    for k in range(KY, NK):
        t_out(k).wait()


def main_call(xT, dyT, w1s, w3s, w2sT, g2):
    def out(n, m, t=BF):
        return jax.ShapeDtypeStruct((n, m), t)

    V = pltpu.VMEM
    return pl.pallas_call(
        main_kernel,
        out_shape=(jax.ShapeDtypeStruct((3, T, FF), BF), out(D, T, F32), out(D, T),
                   out(3 * D, SH, F32), out(3 * D, SH, F32),
                   out(KY * RC, SH), out((NK - KY) * RC, SH), out(KY * RC, SH)),
        in_specs=[ANY] * 6,
        out_specs=(ANY,) * 8,
        scratch_shapes=[
            V((3, D, HB), BF), V((3, D, HB), BF),
            V((2, D, TB), BF), V((2, D, TB), BF), V((TB, D), BF), V((TB, D), BF),
            V((2, TB, HB), BF), V((2, TB, HB), BF), V((2, TB, HB), BF),
            V((2, D, TB), F32), V((2, D, TB), BF),
            V((NK + 2, RC, SH), BF), V((NK, RC, SH), BF),
            V((2, 2, RC, SH), F32), V((4, 2, RC, SH), F32), V((NK, RC, SH), BF),
        ] + [DMA((3,))] * 11 + [DMA((NK,))] * 6 + [DMA((KY,))] * 2
        + [DMA((2, 2)), DMA((4, 2)), DMA((NK,)), DMA((2, 2)), DMA((2, 3, 2)), DMA((2, 2)), DMA((2,))],
        compiler_params=pltpu.CompilerParams(vmem_limit_bytes=VM, collective_id=0, has_side_effects=True),
        cost_estimate=pl.CostEstimate(flops=10 * T * D * FF, bytes_accessed=200_000_000, transcendentals=T * FF),
    )(xT, dyT, w1s, w3s, w2sT, g2)


def gw_kernel(x, dy, act, dxi, gs, ys, dwl, dxo, dwn, lhs, rb, ob, dv, gv, sv, xsem, fsem, ysem, rsem, osem, dsem, gsem, ssem):
    nj, nk, ni, ns = FF // GB, 4, 7, 6
    kc = T // nk

    def col(s):
        return pl.ds(pl.multiple_of(s % nj * GB, 128), GB)

    def x_in(k):
        return pltpu.make_async_copy(x.at[:, k * kc:(k + 1) * kc], lhs.at[0, :, k * kc:(k + 1) * kc], xsem.at[k])

    def first_in(k):
        return pltpu.make_async_copy(act.at[0, k * kc:(k + 1) * kc, 0:GB], rb.at[3, k * kc:(k + 1) * kc], fsem.at[k])

    def tile_in(s, q):
        return pltpu.make_async_copy(act.at[s // nj, :, col(s)], rb.at[q], rsem.at[q])

    def tile_out(s, q):
        return pltpu.make_async_copy(ob.at[q], dwl.at[0, s // nj, :, col(s)], osem.at[q])

    def side_in(u):
        q = u % 2
        r = pl.ds(pl.multiple_of(u * (D // ns), 16), D // ns)
        t = pl.ds(pl.multiple_of(u * (KY * RC // ns), 16), KY * RC // ns)
        return (pltpu.make_async_copy(dxi.at[r, :], dv.at[q], dsem.at[0, q]),
                pltpu.make_async_copy(gs.at[t, :], gv.at[q, 0], gsem.at[q, 0]),
                pltpu.make_async_copy(ys.at[t, :], gv.at[q, 1], gsem.at[q, 1]))

    def dx_out(u):
        r = pl.ds(pl.multiple_of(u * (D // ns), 16), D // ns)
        return pltpu.make_async_copy(dv.at[u % 2], dxo.at[r, :], dsem.at[1, u % 2])

    def n_out(u):
        t = pl.ds(pl.multiple_of(u * (KY * RC // ns), 16), KY * RC // ns)
        return pltpu.make_async_copy(sv.at[u % 2], dwn.at[t, :], ssem.at[u % 2])

    dy_in = pltpu.make_async_copy(dy, lhs.at[1], ysem)
    for k in range(nk):
        x_in(k).start()
        first_in(k).start()
    for t in (0, 1):
        tile_in(1 + t, t).start()
    dy_in.start()
    for k in range(nk):
        x_in(k).wait()
        first_in(k).wait()
        part = jnp.dot(lhs[0, :, k * kc:(k + 1) * kc], rb[3, k * kc:(k + 1) * kc], preferred_element_type=F32)
        ob[3] = part if k == 0 else ob[3] + part
    tile_out(0, 3).start()

    @pl.loop(0, ni)
    def _(u):
        s = 1 + 2 * u
        b = u % 2 * 2

        @pl.when(u < ni - 1)
        def _():
            for t in (0, 1):
                tile_in(s + 2 + t, 2 - b + t).start()

        @pl.when(u >= 2)
        def _():
            dx_out(u - 2).wait()
            tile_out(s, b).wait()

        @pl.when(u >= 3)
        def _():
            n_out(u - 3).wait()

        @pl.when(u >= 1)
        def _():
            tile_out(s, b + 1).wait()

        @pl.when(u < ns)
        def _():
            for cp in side_in(u):
                cp.start()

        @pl.when(u >= 1)
        def _():
            for cp in side_in(u - 1):
                cp.wait()
            dx_out(u - 1).start()

        @pl.when(u == 4)
        def _():
            dy_in.wait()

        for t in (0, 1):
            tile_in(s + t, b + t).wait()
        for t in (0, 1):
            ob[b + t] = jnp.dot(lhs[(s + t) // (2 * nj)], rb[b + t], preferred_element_type=F32)
            if t == 0:
                sv[1 - u % 2] = gv[1 - u % 2, 0].astype(F32) + gv[1 - u % 2, 1].astype(F32)
            tile_out(s + t, b + t).start()

        @pl.when(u >= 1)
        def _():
            n_out(u - 1).start()

    dx_out(ns - 1).wait()
    for k in (ns - 2, ns - 1):
        n_out(k).wait()
    for t in range(4):
        tile_out(t, t).wait()


def gw_call(xT, dyT, act, dxi, gs, ys):
    V, kr = pltpu.VMEM, KY * RC // 6
    return pl.pallas_call(
        gw_kernel,
        out_shape=(jax.ShapeDtypeStruct((1, 3, D, FF), F32), jax.ShapeDtypeStruct((D, T), BF),
                   jax.ShapeDtypeStruct((3 * D, SH), F32)),
        in_specs=[ANY] * 6,
        out_specs=(ANY,) * 3,
        scratch_shapes=[V((2, D, T), BF), V((4, T, GB), BF), V((4, D, GB), F32), V((2, D // 6, T), BF),
                        V((2, 2, kr, SH), BF), V((2, kr, SH), F32),
                        DMA((4,)), DMA((4,)), DMA, DMA((4,)), DMA((4,)), DMA((2, 2)), DMA((2, 2)), DMA((2,))],
        compiler_params=pltpu.CompilerParams(vmem_limit_bytes=VM),
        cost_estimate=pl.CostEstimate(flops=6 * T * D * FF, bytes_accessed=4 * T * D + 6 * T * FF + 12 * D * FF,
                                      transcendentals=0),
    )(xT, dyT, act, dxi, gs, ys)


def final_kernel(g_ref, y_ref, _, o_ref):
    o_ref[...] = g_ref[...].astype(F32) + y_ref[...].astype(F32)


def final_call(gt, yt, acc):
    rb, first = 2 * RC, KY // 2
    spec = pl.BlockSpec((rb, SH), lambda i: (i, 0))
    return pl.pallas_call(
        final_kernel,
        out_shape=jax.ShapeDtypeStruct((3 * D, SH), F32),
        grid=((NK - KY) * RC // rb,), in_specs=[spec, spec, ANY],
        out_specs=pl.BlockSpec((rb, SH), lambda i: (i + first, 0)),
        input_output_aliases={2: 0},
        compiler_params=pltpu.CompilerParams(vmem_limit_bytes=VM),
        cost_estimate=pl.CostEstimate(flops=D * SH, bytes_accessed=8 * D * SH, transcendentals=0),
    )(gt, yt, acc)


def solution(mesh):
    grp = ("fo", "fi")
    alla = ("dp", "fo", "fi")
    flip = [(0, 1), (1, 0)]

    def local(x, dy, w1s, w3s, w2s, g):
        xT, dyT = x.T, dy.T
        act, _, dxT, _, _, gs, gt, ys = main_call(xT, dyT, w1s, w3s, w2s.T, g.reshape(3 * D, FF))
        yt = lax.ppermute(gt, "dp", flip)
        dwl, dxT, dwn = gw_call(xT, dyT, act, dxT, gs, ys)
        yt, dwn = lax.optimization_barrier((yt, dwn))
        dwn = final_call(gt, yt, dwn).reshape(3, D, SH)
        return dxT.T, dwn, dwl

    return jax.shard_map(
        local, mesh=mesh,
        in_specs=(P(alla, None), P(alla, None), P(None, grp), P(None, grp), P(grp, None),
                  P(alla, None, None, None)),
        out_specs=(P(alla, None), P(None, None, grp), P(alla, None, None, None)),
        check_vma=False)
```
